32 devices in a mesh: gz: 8 (over y, x, core), gy: 4 (over z).
Axes of the slice: x: 2, y: 2, z: 4, core: 2. Of those that a mesh axis runs over, the one named last changes fastest.
Arguments:
- features: bfloat16 [32, 32, 32, 256], P(None, 'gz', 'gy'), may hold values from -6 to 6
- scale_first: float32 [32], replicated, may hold values from 0.5 to 2
- shift_first: float32 [32], replicated, may hold values from -3 to 3
- conv_first: bfloat16 [3, 3, 32, 32], replicated, may hold values from -0.375 to 0.375
- bias_first: float32 [32], replicated, may hold values from -3 to 3
- scale_second: float32 [32], replicated, may hold values from 0.5 to 2
- shift_second: float32 [32], replicated, may hold values from -3 to 3
- conv_second: bfloat16 [3, 3, 32, 32], replicated, may hold values from -0.375 to 0.375
- bias_second: float32 [32], replicated, may hold values from -3 to 3
- flow_weight: bfloat16 [2, 32], replicated, may hold values from -1 to 1
Outputs:
- smoothed: float32 [3, 32, 32, 256], P(None, 'gz', 'gy')
The draws below stay inside these ranges and needn't reach their ends.
All inputs are finite; a program needn't handle non-finite values.
Results may differ from the reference program's by a relative error of at most 0.0015.
Values may be sent and summed in bfloat16 or wider, within the bound.
No kernel may reach another device: no remote copies, remote signals or barrier semaphores. Data moves between devices by JAX's collectives and lax.ppermute only.
A program may use at most 64 MiB of HBM per device.

```python
import math
import jax
import jax.numpy as jnp
from jax import lax

C = 32
NX = 256
NZ = 32
NY = 32


def block_scale(rng, dims, shards, least, largest):
    loudness = 1.0
    for position, blocks in shards:
        steps = jax.random.uniform(jax.random.fold_in(jax.random.fold_in(rng, 6), position), (blocks,), jnp.float32, least / len(shards), largest / len(shards))
        loudness = loudness * jnp.repeat(jnp.exp(steps), dims[position] // blocks).reshape((-1,) + (1,) * (len(dims) - 1 - position))
    return loudness


def normal_values(rng, shape, spread, limit, split=(), kind=jnp.bfloat16):
    drawn = spread * jax.random.normal(rng, shape, jnp.float32)
    if split:
        drawn = drawn * block_scale(rng, shape, split, -0.22, 0.18)
    return jnp.clip(drawn, -limit, limit).astype(kind)


def setup_inputs(seed: int = 0) -> dict:
    key_of = jax.random.split(jax.random.key(seed), 11)
    features = normal_values(key_of[0], (C, NZ, NY, NX), 1.0, 6.0, ((1, 8), (2, 4)))
    scale_first = jnp.clip(jnp.exp(jax.random.uniform(key_of[1], (C,), jnp.float32, math.log(0.5), math.log(2.0))), 0.5, 2.0)
    shift_first = normal_values(key_of[2], (C,), 0.5, 3.0, (), jnp.float32)
    conv_first = normal_values(key_of[3], (3, 3, C, C), (9 * C) ** -0.5, 0.375)
    bias_first = normal_values(key_of[4], (C,), 0.5, 3.0, (), jnp.float32)
    scale_second = jnp.clip(jnp.exp(jax.random.uniform(key_of[5], (C,), jnp.float32, math.log(0.5), math.log(2.0))), 0.5, 2.0)
    shift_second = normal_values(key_of[6], (C,), 0.5, 3.0, (), jnp.float32)
    conv_second = normal_values(key_of[7], (3, 3, C, C), (9 * C) ** -0.5, 0.375)
    bias_second = normal_values(key_of[8], (C,), 0.5, 3.0, (), jnp.float32)
    flow_weight = normal_values(key_of[9], (2, C), C ** -0.5, 1.0)
    return {"features": features, "scale_first": scale_first, "shift_first": shift_first, "conv_first": conv_first, "bias_first": bias_first, "scale_second": scale_second, "shift_second": shift_second, "conv_second": conv_second, "bias_second": bias_second, "flow_weight": flow_weight}


def shift_cols(source, delta):
    if delta == 0:
        return source
    zeros = jnp.zeros(source.shape[:-1] + (1,), source.dtype)
    if delta == 1:
        return jnp.concatenate([source[..., 1:], zeros], -1)
    return jnp.concatenate([zeros, source[..., :-1]], -1)


def plane_conv(source, weight, plane_axes, count_z, count_y, start_z, start_y):
    summed = None
    for row_tap in range(3):
        for col_tap in range(3):
            offset = {1: 0, 2: 0, 3: 0}
            offset[plane_axes[0]] = row_tap - 1
            offset[plane_axes[1]] = col_tap - 1
            low_z = start_z + offset[1]
            low_y = start_y + offset[2]
            window = lax.slice(source, (0, low_z, low_y, 0), (source.shape[0], low_z + count_z, low_y + count_y, source.shape[3]))
            window = shift_cols(window, offset[3])
            term = jnp.einsum('oc,czyx->ozyx', weight[row_tap, col_tap].astype(jnp.float32), window.astype(jnp.float32), preferred_element_type=jnp.float32)
            summed = term if summed is None else summed + term
    return summed


def column(vector):
    return vector[:, None, None, None]


def reference(features, scale_first, shift_first, conv_first, bias_first, scale_second, shift_second, conv_second, bias_second, flow_weight):
    depth, rows = features.shape[1], features.shape[2]
    unit = jax.nn.relu(features.astype(jnp.float32) * column(scale_first) + column(shift_first)).astype(jnp.bfloat16)
    padded = jnp.pad(unit, ((0, 0), (1, 1), (1, 1), (0, 0)))
    flows = []
    for plane_axes in ((2, 3), (1, 3), (1, 2)):
        hidden = plane_conv(padded, conv_first, plane_axes, depth, rows, 1, 1) + column(bias_first)
        active = jax.nn.relu(hidden * column(scale_second) + column(shift_second)).astype(jnp.bfloat16)
        active = jnp.pad(active, ((0, 0), (1, 1), (1, 1), (0, 0)))
        output = plane_conv(active, conv_second, plane_axes, depth, rows, 1, 1)
        block = (output + column(bias_second) + features.astype(jnp.float32)).astype(jnp.bfloat16)
        flows.append(jnp.einsum('kc,czyx->kzyx', flow_weight.astype(jnp.float32), block.astype(jnp.float32), preferred_element_type=jnp.float32))
    flow_xy, flow_xz, flow_yz = flows
    mean_flow = jnp.stack([0.5 * (flow_xz[0] + flow_yz[0]), 0.5 * (flow_xy[0] + flow_yz[1]), 0.5 * (flow_xy[1] + flow_xz[1])])
    ext = jnp.pad(mean_flow, ((0, 0), (1, 1), (1, 1), (0, 0)))
    ext = 0.25 * ext[:, :-2] + 0.5 * ext[:, 1:-1] + 0.25 * ext[:, 2:]
    ext = 0.25 * ext[:, :, :-2] + 0.5 * ext[:, :, 1:-1] + 0.25 * ext[:, :, 2:]
    return 0.25 * shift_cols(ext, -1) + 0.5 * ext + 0.25 * shift_cols(ext, 1)
```

```python
import functools

import jax
import jax.numpy as jnp
from jax import lax
from jax.experimental import pallas as pl
from jax.experimental.pallas import tpu as pltpu
from jax.sharding import PartitionSpec as P


HALO = 3
SPAN = 6
WIDE = SPAN + 2
F32, BF16 = jnp.float32, jnp.bfloat16
VMEM = pl.BlockSpec(memory_space=pltpu.VMEM)
HBM = pl.BlockSpec(memory_space=pltpu.HBM)


def iota(shape, dim):
    return lax.broadcasted_iota(jnp.int32, shape, dim)


def matmul(a, b):
    return jnp.dot(a, b, preferred_element_type=F32)


def swap(value, axis, first):
    pairs = []
    for i in range(first, lax.axis_size(axis) - 1, 2):
        pairs += [(i, i + 1), (i + 1, i)]
    return lax.ppermute(value, axis, pairs)


def call(kernel, outs, args, flops, mib, scratch=(), space=VMEM):
    nbytes = sum(a.size * a.dtype.itemsize for a in (*outs, *args))
    return pl.pallas_call(
        kernel,
        out_shape=outs,
        in_specs=[space] * len(args),
        out_specs=[VMEM] * len(outs),
        scratch_shapes=list(scratch),
        cost_estimate=pl.CostEstimate(flops=flops, bytes_accessed=nbytes, transcendentals=0),
        compiler_params=pltpu.CompilerParams(vmem_limit_bytes=mib * 2**20),
    )(*args)


def odd(axis):
    return lax.rem(lax.axis_index(axis), 2)


def pack_kernel(feat_ref, own_ref, far_ref, even_ref, odd_ref):
    channels, depth, rows, cols = feat_ref.shape
    size = channels * rows
    row, col = iota((size, size), 0), iota((size, size), 1)
    order = ((row // channels == col % rows) & (row % channels == col // rows)).astype(F32).astype(BF16)
    part_z, part_y = odd("gz"), odd("gy")
    for z in range(depth):
        value = feat_ref[:, z].astype(F32).reshape(size, cols).astype(BF16)
        value = matmul(order, value).astype(BF16).reshape(rows, channels, cols)
        own_ref[part_z * z + (1 - part_z) * (depth - 1 - z)] = value
    first_even, first_odd = (1 - part_y) * (rows - HALO), part_y * (rows - HALO)
    for layer in range(HALO):
        far_ref[layer] = own_ref[depth - 1 - layer]
    for z in range(depth):
        for row in range(HALO):
            even_ref[z, row] = own_ref[z, first_even + row]
            odd_ref[z, row] = own_ref[z, first_odd + row]


def rim_kernel(own_ref, even_ref, odd_ref, near_ref, corner_ref):
    depth, rows = own_ref.shape[:2]
    for layer in range(HALO):
        near_ref[layer, :rows] = own_ref[layer]
        near_ref[layer, rows : rows + HALO] = even_ref[layer]
        near_ref[layer, rows + HALO :] = odd_ref[layer]
        corner_ref[layer, :HALO] = even_ref[depth - 1 - layer]
        corner_ref[layer, HALO:] = odd_ref[depth - 1 - layer]


def weights_kernel(
    scale1_hbm, shift1_hbm, conv1_hbm, bias1_hbm, scale2_hbm, shift2_hbm, conv2_hbm, bias2_hbm, flow_hbm,
    wxy_ref, wyz_ref, wza_ref, wzb_ref, vxy_ref, vyz_ref, vza_ref, vzb_ref, vf_ref,
    s1_ref, t1_ref, s2_ref, t2_ref, const_ref,
    scale1, shift1, conv1, bias1, scale2, shift2, conv2, bias2, flow, taps, folds, sem,
):
    copies = [
        pltpu.make_async_copy(source, target, sem.at[n])
        for n, (source, target) in enumerate(
            (
                (scale1_hbm, scale1), (shift1_hbm, shift1), (conv1_hbm, conv1), (bias1_hbm, bias1),
                (scale2_hbm, scale2), (shift2_hbm, shift2), (conv2_hbm, conv2), (bias2_hbm, bias2), (flow_hbm, flow),
            )
        )
    ]
    for copy in copies:
        copy.start()
    for copy in copies:
        copy.wait()
    c = conv1.shape[-1]
    part_z = odd("gz")

    def along_z(i):
        return part_z * i + (1 - part_z) * (2 - i)

    def spread(vector, rows, cols):
        pick = iota((rows, c), 0) % c == iota((rows, c), 1)
        column = jnp.sum(jnp.where(pick, vector, 0.0), axis=1, keepdims=True)
        return jnp.broadcast_to(column, (rows, cols))

    s1_ref[...] = spread(scale1[...], *s1_ref.shape)
    t1_ref[...] = spread(shift1[...], *t1_ref.shape)
    s2_ref[...] = spread(scale2[...], *s2_ref.shape)
    t2_ref[...] = spread(bias1[...] * scale2[...] + shift2[...], *t2_ref.shape)
    const = jnp.sum(flow[...].astype(F32) * bias2[...], axis=1, keepdims=True)
    half = const_ref.shape[0] // 2
    for k in range(2):
        const_ref[k * half : (k + 1) * half] = jnp.broadcast_to(const[k : k + 1], (half, const_ref.shape[1]))

    def tile_of(cols):
        return (iota((c, cols), 0) == iota((c, cols), 1) % c).astype(F32).astype(BF16)

    tile = tile_of(taps.shape[-1])
    short = tile_of(folds.shape[-1])
    for i in range(3):
        for j in range(3):
            taps[i, j] = matmul(conv1[i, j], tile)
            both = matmul(flow[...], conv2[i, j])
            high = both.astype(BF16)
            low = (both - high.astype(F32)).astype(BF16)
            folds[i, j, 0] = matmul(high, short)
            folds[i, j, 1] = matmul(low, short)

    def banded(ref, pick):
        rows, cols = ref.shape
        group = cols // 3
        lane = iota((c, cols), 1)
        slot = lane % group // c
        for a in range(rows // c):
            value = jnp.zeros((c, cols), F32)
            for g in range(3):
                for i in range(3):
                    value = jnp.where((slot == a + i) & (lane // group == g), pick(g, i)[:, :cols], value)
            ref[a * c : (a + 1) * c] = value.astype(BF16)

    banded(wxy_ref, lambda g, i: taps[i, g])
    banded(wyz_ref, lambda g, i: taps[along_z(g), i])
    banded(wza_ref, lambda g, i: taps[along_z(i), g])
    banded(wzb_ref, lambda g, i: taps[along_z(i), g])

    def banded_flow(ref, pick, skip):
        cols = ref.shape[1]
        height = ref.shape[0] // 12
        band = iota((height, cols), 1) // c + skip - iota((height, cols), 0)
        for part in range(2):
            for g in range(3):
                for k in range(2):
                    block = jnp.zeros((height, cols), F32)
                    for i in range(3):
                        row, col = pick(g, i)
                        block = jnp.where(band == i, folds[row, col, part, k : k + 1, :cols], block)
                    at = ((part * 3 + g) * 2 + k) * height
                    ref[at : at + height] = block.astype(BF16)

    banded_flow(vxy_ref, lambda g, i: (i, g), 0)
    banded_flow(vyz_ref, lambda g, i: (along_z(g), i), 0)
    banded_flow(vza_ref, lambda g, i: (along_z(i), g), 0)
    banded_flow(vzb_ref, lambda g, i: (along_z(i), g), vza_ref.shape[1] // c)
    cols = vf_ref.shape[1]
    plain = matmul(flow[...], short)
    for k in range(2):
        band = iota((half, cols), 1) // c - iota((half, cols), 0)
        vf_ref[k * half : (k + 1) * half] = jnp.where(band == 0, plain[k : k + 1, :cols], 0.0).astype(BF16)


def shift_right(value):
    return jnp.where(iota(value.shape, 1) == 0, 0.0, pltpu.roll(value, 1, 1))


def shift_left(value):
    last = value.shape[1] - 1
    return jnp.where(iota(value.shape, 1) == last, 0.0, pltpu.roll(value, last, 1))


def valid_sides():
    part_z = odd("gz")
    low = (lax.axis_index("gz") > 0).astype(F32)
    high = (lax.axis_index("gz") < lax.axis_size("gz") - 1).astype(F32)
    near = jnp.where(part_z == 1, low, high)
    far = jnp.where(part_z == 1, high, low)
    low_y = (lax.axis_index("gy") > 0).astype(F32)
    high_y = (lax.axis_index("gy") < lax.axis_size("gy") - 1).astype(F32)
    return near, far, low_y, high_y


def y_halos(rows, low_y, high_y):
    part_y = odd("gy")
    valid_even = jnp.where(part_y == 1, low_y, high_y)
    valid_odd = jnp.where(part_y == 1, high_y, low_y)
    return ((1 - part_y) * (rows + HALO), valid_even), (part_y * (rows + HALO), valid_odd)


def normalized(value, s1, t1, valid):
    count, c, cols = value.shape
    size = count * c
    value = jnp.maximum(value.reshape(size, cols).astype(F32) * s1[:size] + t1[:size], 0.0)
    if valid is not None:
        value = value * valid
    return [v.astype(BF16).reshape(count, c, cols) for v in (shift_right(value), value, shift_left(value))]


def set_masks(sm, tm, s2, t2, low_y, high_y):
    size, cols = s2.shape
    c = size // SPAN
    row = iota((size, cols), 0)
    for n, keep in enumerate((row >= 2 * c, row < size - 2 * c)):
        keep = jnp.where(keep, 1.0, high_y if n else low_y)
        sm[n] = s2[...] * keep
        tm[n] = t2[...] * keep


def activate(hidden, scale, shift, c, valid=None):
    value = jnp.maximum(hidden * scale + shift, 0.0)
    if valid is not None:
        value = value * valid
    return value.astype(BF16).reshape(-1, c, value.shape[1])


def stack(pieces):
    return jnp.concatenate([p.reshape(-1, p.shape[-1]) for p in pieces], axis=0)


def two_parts(value):
    half = value.shape[0] // 2
    return value[:half] + value[half:]


def along_x(value):
    value = two_parts(value)
    step = value.shape[0] // 3
    return shift_right(value[:step]) + value[step : 2 * step] + shift_left(value[2 * step :])


def planes(
    unit, xy_layers, out_layers, out_xz, data_xz, edge_xz,
    wxy, wyz, wz, vxy, vyz, vz, s2, t2, sm, tm, act_xy, act_yz, act_xz, fxz, outer,
):
    c, cols = act_xy.shape[-2:]
    wide = act_xy.shape[1]
    flow_xy, flow_yz = {}, {}
    for n, z in enumerate(xy_layers):
        for w in range(wide // SPAN):
            data = stack([unit(j, z, slice(w * SPAN, w * SPAN + WIDE)) for j in range(3)])
            act_xy[n, w * SPAN : (w + 1) * SPAN] = activate(matmul(wxy[...], data), sm[w], tm[w], c)
    for n, z in enumerate(out_layers):
        for w in range(wide // SPAN):
            data = stack([unit(1, z + i - 1, slice(w * SPAN, w * SPAN + WIDE)) for i in range(3)])
            act_yz[n, w * SPAN : (w + 1) * SPAN] = activate(matmul(wyz[...], data), sm[w], tm[w], c, outer(z))
    count = len(out_xz)
    row = iota((count * c, cols), 0)
    keep = jnp.where((row >= edge_xz[0] * c) & (row < edge_xz[1] * c), edge_xz[2], 1.0)
    scale, shift = s2[: count * c] * keep, t2[: count * c] * keep
    for y in range(act_xz.shape[0]):
        data = stack([unit(j, z, y + 2) for j in range(3) for z in data_xz])
        act_xz[y] = activate(matmul(wz[...], data), scale, shift, c)
    for y in range(act_xz.shape[0]):
        flow = along_x(matmul(vz[...], act_xz[y].reshape(-1, cols)))
        half = flow.shape[0] // 2
        for k in range(2):
            fxz[k, :, y, :] = flow[k * half : (k + 1) * half]
    for n, z in enumerate(xy_layers):
        flow_xy[z] = along_x(matmul(vxy[...], act_xy[n].reshape(-1, cols)))
    for n, z in enumerate(out_layers):
        value = two_parts(matmul(vyz[...], act_yz[n].reshape(-1, cols)))
        step = value.shape[0] // 3
        flow_yz[z] = [value[i * step : (i + 1) * step] for i in range(3)]
    return flow_xy, flow_yz


def gather_mean(add, layer, fxz, flow_xy, flow_yz, base, height):
    at = layer - 2
    parts = [0.5 * fxz[0, at], None, 0.5 * fxz[1, at]]

    def plus(k, value):
        parts[k] = value if parts[k] is None else parts[k] + value

    for i in range(3):
        if layer + i - 1 in flow_yz:
            piece = 0.5 * flow_yz[layer + i - 1][i]
            plus(0, piece[:height])
            plus(1, piece[height:])
    if layer in flow_xy:
        piece = 0.5 * flow_xy[layer]
        plus(1, piece[:height])
        plus(2, piece[height:])
    if base is not None:
        plus(0, base[:height])
        plus(1, 0.5 * (base[:height] + base[height:]))
        plus(2, base[height:])
    for k in range(3):
        if parts[k] is not None:
            add(k, at, parts[k])


def near_kernel(
    own, near, yeven, yodd, wxy, wyz, wz, vxy, vyz, vz, vf, s1, t1, s2, t2, const,
    mean, tail, unit, feat, act_xy, act_yz, act_xz, sm, tm, fxz,
):
    depth, rows, _, cols = own.shape
    valid_near, _, low_y, high_y = valid_sides()
    (at_even, valid_even), (at_odd, valid_odd) = y_halos(rows, low_y, high_y)
    first = HALO + depth - 2

    def place(value, z, y, valid):
        count = value.shape[0]
        if z >= HALO - 1:
            feat[z - HALO + 1, pl.ds(y, count)] = value
        for j, moved in enumerate(normalized(value, s1, t1, valid)):
            if z < first:
                unit[j, z, pl.ds(y, count)] = moved
            else:
                tail[j, z - first, pl.ds(y, count)] = moved

    for z in range(depth):
        place(own[z], HALO + z, HALO, None)
        place(yeven[z], HALO + z, at_even, valid_even)
        place(yodd[z], HALO + z, at_odd, valid_odd)
    for z in range(HALO):
        place(near[z, :rows], HALO - 1 - z, HALO, valid_near)
        place(near[z, rows : rows + HALO], HALO - 1 - z, at_even, valid_near * valid_even)
        place(near[z, rows + HALO :], HALO - 1 - z, at_odd, valid_near * valid_odd)
    set_masks(sm, tm, s2, t2, low_y, high_y)

    def read(j, z, y):
        return unit[j, z, y] if z < first else tail[j, z - first, y]

    outs = list(range(1, depth + 2))
    flow_xy, flow_yz = planes(
        read, list(range(2, depth + 3)), outs, outs, list(range(depth + 3)), (0, 2, valid_near),
        wxy, wyz, wz, vxy, vyz, vz, s2, t2, sm, tm, act_xy, act_yz, act_xz, fxz,
        lambda z: valid_near if z < HALO else None,
    )
    height = mean.shape[2]

    def store(k, at, value):
        mean[k, at] = value

    for layer in range(2, depth + 3):
        base = matmul(vf[...], feat[layer - 2, 2 : rows + 4].reshape(-1, cols)) + const[...]
        gather_mean(store, layer, fxz, flow_xy, flow_yz, base, height)


def far_kernel(
    far, corner, tail, mean, wxy, wyz, wz, vxy, vyz, vz, vf, s1, t1, s2, t2, const,
    out, unit, act_xy, act_yz, act_xz, sm, tm, fxz, feat, total,
):
    _, depth, rows, cols = out.shape
    valid_near, valid_far, low_y, high_y = valid_sides()
    (at_even, valid_even), (at_odd, valid_odd) = y_halos(rows, low_y, high_y)
    start = HALO + depth
    first = start - 2

    def place(value, z, y, valid):
        count = value.shape[0]
        if z == 0:
            feat[pl.ds(y, count)] = value
        for j, moved in enumerate(normalized(value, s1, t1, valid)):
            unit[j, z, pl.ds(y, count)] = moved

    for z in range(HALO):
        place(far[z], z, HALO, valid_far)
        place(corner[z, :HALO], z, at_even, valid_far * valid_even)
        place(corner[z, HALO:], z, at_odd, valid_far * valid_odd)
    set_masks(sm, tm, s2, t2, low_y, high_y)

    def read(j, z, y):
        return unit[j, z - start, y] if z >= start else tail[j, z - first, y]

    outs = list(range(start - 1, start + 2))
    flow_xy, flow_yz = planes(
        read, [start], outs, outs, list(range(first, start + HALO)), (1, 3, valid_far),
        wxy, wyz, wz, vxy, vyz, vz, s2, t2, sm, tm, act_xy, act_yz, act_xz, fxz,
        lambda z: valid_far if z >= start else None,
    )
    height = mean.shape[2]
    spot = iota((height, cols), 0)
    inside_y = jnp.where(spot == 0, low_y, jnp.where(spot == rows + 1, high_y, jnp.where(spot < rows + 1, 1.0, 0.0)))

    def store(k, at, value):
        if at < depth + 1:
            value = value + mean[k, at]
        total[k, at] = value * (inside_y * valid_far if at == depth + 1 else inside_y)

    for k in range(3):
        for at in range(depth - 1):
            total[k, at] = mean[k, at] * (inside_y * valid_near if at == 0 else inside_y)
    for layer in range(first, start + 1):
        base = None
        if layer == start:
            base = matmul(vf[...], feat[2 : rows + 4].reshape(-1, cols)) + const[...]
        gather_mean(store, layer, fxz, flow_xy, flow_yz, base, height)
    part_z = odd("gz")
    for k in range(3):
        for z in range(depth):
            value = 0.25 * (total[k, z] + total[k, z + 2]) + 0.5 * total[k, z + 1]
            value = 0.25 * (value[:rows] + value[2 : rows + 2]) + 0.5 * value[1 : rows + 1]
            value = 0.25 * (shift_right(value) + shift_left(value)) + 0.5 * value
            out[k, part_z * z + (1 - part_z) * (depth - 1 - z)] = value


def shards(
    features, scale_first, shift_first, conv_first, bias_first,
    scale_second, shift_second, conv_second, bias_second, flow_weight,
):
    c, depth, rows, cols = features.shape
    shape = jax.ShapeDtypeStruct
    cells = functools.partial(shape, dtype=BF16)
    side = cells((depth, HALO, c, cols))
    own, send_far, send_even, send_odd = call(
        pack_kernel,
        [cells((depth, rows, c, cols)), cells((HALO, rows, c, cols)), side, side],
        [features], 2 * features.size * c * rows, 6,
    )
    far = swap(send_far, "gz", 1)
    yeven = swap(send_even, "gy", 0)
    yodd = swap(send_odd, "gy", 1)

    broad = rows + 2 * HALO
    high = -(-(rows + 2) // 8) * 8
    deep = -(-(depth + 2) // 8) * 8
    params = [
        scale_first[None], shift_first[None], conv_first, bias_first[None],
        scale_second[None], shift_second[None], conv_second, bias_second[None], flow_weight,
    ]
    params = [pltpu.with_memory_space_constraint(p, pltpu.HBM) for p in params]
    wxy, wyz, wza, wzb, vxy, vyz, vza, vzb, *rest = call(
        weights_kernel,
        [
            cells((SPAN * c, 3 * WIDE * c)),
            cells((SPAN * c, 3 * WIDE * c)),
            cells(((depth + 1) * c, 3 * (depth + 3) * c)),
            cells((HALO * c, 3 * (HALO + 2) * c)),
            cells((12 * high, (rows + 4) * c)),
            cells((12 * high, (rows + 4) * c)),
            cells((12 * deep, (depth + 1) * c)),
            cells((12 * deep, HALO * c)),
            cells((2 * high, (rows + 2) * c)),
            shape((rows * c, cols), F32),
            shape((rows * c, cols), F32),
            shape((SPAN * c, cols), F32),
            shape((SPAN * c, cols), F32),
            shape((2 * high, cols), F32),
        ],
        params,
        2 * 10**9, 10,
        [
            *(pltpu.VMEM(p.shape, p.dtype) for p in params),
            pltpu.VMEM((3, 3, c, 3 * WIDE * c), F32),
            pltpu.VMEM((3, 3, 2, 2, (rows + 4) * c), F32),
            pltpu.SemaphoreType.DMA((len(params),)),
        ],
        HBM,
    )
    send_near, send_corner = call(
        rim_kernel,
        [cells((HALO, broad, c, cols)), cells((HALO, 2 * HALO, c, cols))],
        [own, yeven, yodd], 10**6, 5,
    )
    corner = swap(send_corner, "gz", 1)
    near = swap(send_near, "gz", 0)

    def scratch(layers_xy, layers_out):
        return [
            pltpu.VMEM((layers_xy, rows + 4, c, cols), BF16),
            pltpu.VMEM((layers_out, rows + 4, c, cols), BF16),
            pltpu.VMEM((rows + 2, layers_out, c, cols), BF16),
            pltpu.VMEM((2, SPAN * c, cols), F32),
            pltpu.VMEM((2, SPAN * c, cols), F32),
            pltpu.VMEM((2, deep, high, cols), F32),
        ]

    mean, tail = call(
        near_kernel,
        [shape((3, depth + 1, high, cols), F32), cells((3, 2, broad, c, cols))],
        [own, near, yeven, yodd, wxy, wyz, wza, vxy, vyz, vza, *rest],
        6 * 10**9, 24,
        [
            pltpu.VMEM((3, depth + 1, broad, c, cols), BF16),
            pltpu.VMEM((depth + 1, broad, c, cols), BF16),
            *scratch(depth + 1, depth + 1),
        ],
    )
    (out,) = call(
        far_kernel,
        [shape((3, depth, rows, cols), F32)],
        [far, corner, tail, mean, wxy, wyz, wzb, vxy, vyz, vzb, *rest],
        2 * 10**9, 16,
        [
            pltpu.VMEM((3, HALO, broad, c, cols), BF16),
            *scratch(1, HALO),
            pltpu.VMEM((broad, c, cols), BF16),
            pltpu.VMEM((3, depth + 2, high, cols), F32),
        ],
    )
    return out


def solution(mesh):
    return jax.shard_map(
        shards,
        mesh=mesh,
        in_specs=(P(None, "gz", "gy", None), P(), P(), P(), P(), P(), P(), P(), P(), P()),
        out_specs=P(None, "gz", "gy", None),
        check_vma=False,
    )
```

```python
import functools

import jax
import jax.numpy as jnp
from jax import lax
from jax.experimental import pallas as pl
from jax.experimental.pallas import tpu as pltpu
from jax.sharding import PartitionSpec as P


HALO = 3
SPAN = 6
WIDE = SPAN + 2
EDGE = 3
F32, BF16 = jnp.float32, jnp.bfloat16
VMEM = pl.BlockSpec(memory_space=pltpu.VMEM)
HBM = pl.BlockSpec(memory_space=pltpu.HBM)


def iota(shape, dim):
    return lax.broadcasted_iota(jnp.int32, shape, dim)


def matmul(a, b):
    return jnp.dot(a, b, preferred_element_type=F32)


def swap(value, axis, first):
    pairs = []
    for i in range(first, lax.axis_size(axis) - 1, 2):
        pairs += [(i, i + 1), (i + 1, i)]
    return lax.ppermute(value, axis, pairs)


def call(kernel, outs, args, flops, mib, scratch=(), space=VMEM):
    nbytes = sum(a.size * a.dtype.itemsize for a in (*outs, *args))
    return pl.pallas_call(
        kernel,
        out_shape=outs,
        in_specs=[space] * len(args),
        out_specs=[VMEM] * len(outs),
        scratch_shapes=list(scratch),
        cost_estimate=pl.CostEstimate(flops=flops, bytes_accessed=nbytes, transcendentals=0),
        compiler_params=pltpu.CompilerParams(vmem_limit_bytes=mib * 2**20),
    )(*args)


def odd(axis):
    return lax.rem(lax.axis_index(axis), 2)


def cell_order(channels, rows):
    size = channels * rows
    row, col = iota((size, size), 0), iota((size, size), 1)
    return ((row // channels == col % rows) & (row % channels == col // rows)).astype(F32).astype(BF16)


def pack_kernel(feat_ref, own_ref, even_ref, odd_ref, far_ref):
    channels, depth, rows, cols = feat_ref.shape
    size = channels * rows
    order = cell_order(channels, rows)
    part_z, part_y = odd("gz"), odd("gy")
    for z in range(depth):
        value = feat_ref[:, z].astype(F32).reshape(size, cols).astype(BF16)
        value = matmul(order, value).astype(BF16).reshape(rows, channels, cols)
        own_ref[part_z * z + (1 - part_z) * (depth - 1 - z)] = value
    first_even, first_odd = (1 - part_y) * (rows - HALO), part_y * (rows - HALO)
    for z in range(depth):
        for row in range(HALO):
            even_ref[z, row] = own_ref[z, first_even + row]
            odd_ref[z, row] = own_ref[z, first_odd + row]
    for layer in range(HALO):
        far_ref[layer] = own_ref[depth - 1 - layer]


def weights_kernel(
    scale1_hbm, shift1_hbm, conv1_hbm, bias1_hbm, scale2_hbm, shift2_hbm, conv2_hbm, bias2_hbm, flow_hbm,
    wxy_ref, wyz_ref, wza_ref, wzb_ref, wxe_ref, wye_ref,
    vxy_ref, vyz_ref, vza_ref, vzb_ref, vxe_ref, vye_ref, vf_ref,
    s1_ref, t1_ref, s2_ref, t2_ref, const_ref,
    scale1, shift1, conv1, bias1, scale2, shift2, conv2, bias2, flow, taps, folds, sem,
):
    copies = [
        pltpu.make_async_copy(source, target, sem.at[n])
        for n, (source, target) in enumerate(
            (
                (scale1_hbm, scale1), (shift1_hbm, shift1), (conv1_hbm, conv1), (bias1_hbm, bias1),
                (scale2_hbm, scale2), (shift2_hbm, shift2), (conv2_hbm, conv2), (bias2_hbm, bias2), (flow_hbm, flow),
            )
        )
    ]
    for copy in copies:
        copy.start()
    for copy in copies:
        copy.wait()
    c = conv1.shape[-1]
    part_z = odd("gz")

    def along_z(i):
        return part_z * i + (1 - part_z) * (2 - i)

    def spread(vector, rows, cols):
        pick = iota((rows, c), 0) % c == iota((rows, c), 1)
        column = jnp.sum(jnp.where(pick, vector, 0.0), axis=1, keepdims=True)
        return jnp.broadcast_to(column, (rows, cols))

    s1_ref[...] = spread(scale1[...], *s1_ref.shape)
    t1_ref[...] = spread(shift1[...], *t1_ref.shape)
    s2_ref[...] = spread(scale2[...], *s2_ref.shape)
    t2_ref[...] = spread(bias1[...] * scale2[...] + shift2[...], *t2_ref.shape)
    const = jnp.sum(flow[...].astype(F32) * bias2[...], axis=1, keepdims=True)
    half = const_ref.shape[0] // 2
    for k in range(2):
        const_ref[k * half : (k + 1) * half] = jnp.broadcast_to(const[k : k + 1], (half, const_ref.shape[1]))

    def tile_of(cols):
        return (iota((c, cols), 0) == iota((c, cols), 1) % c).astype(F32).astype(BF16)

    tile = tile_of(taps.shape[-1])
    short = tile_of(folds.shape[-1])
    for i in range(3):
        for j in range(3):
            taps[i, j] = matmul(conv1[i, j], tile)
            both = matmul(flow[...], conv2[i, j])
            high = both.astype(BF16)
            low = (both - high.astype(F32)).astype(BF16)
            folds[i, j, 0] = matmul(high, short)
            folds[i, j, 1] = matmul(low, short)

    def banded(ref, pick):
        rows, cols = ref.shape
        group = cols // 3
        lane = iota((c, cols), 1)
        slot = lane % group // c
        for a in range(rows // c):
            value = jnp.zeros((c, cols), F32)
            for g in range(3):
                for i in range(3):
                    value = jnp.where((slot == a + i) & (lane // group == g), pick(g, i)[:, :cols], value)
            ref[a * c : (a + 1) * c] = value.astype(BF16)

    banded(wxy_ref, lambda g, i: taps[i, g])
    banded(wyz_ref, lambda g, i: taps[along_z(g), i])
    banded(wza_ref, lambda g, i: taps[along_z(i), g])
    banded(wzb_ref, lambda g, i: taps[along_z(i), g])
    banded(wxe_ref, lambda g, i: taps[i, g])
    banded(wye_ref, lambda g, i: taps[along_z(g), i])

    def banded_flow(ref, pick, place):
        cols = ref.shape[1]
        height = ref.shape[0] // 12
        band = place(iota((height, cols), 1) // c) - iota((height, cols), 0)
        for part in range(2):
            for g in range(3):
                for k in range(2):
                    block = jnp.zeros((height, cols), F32)
                    for i in range(3):
                        row, col = pick(g, i)
                        block = jnp.where(band == i, folds[row, col, part, k : k + 1, :cols], block)
                    at = ((part * 3 + g) * 2 + k) * height
                    ref[at : at + height] = block.astype(BF16)

    middle = vxy_ref.shape[1] // c - 2 * EDGE
    past = vza_ref.shape[1] // c
    banded_flow(vxy_ref, lambda g, i: (i, g), lambda b: b)
    banded_flow(vyz_ref, lambda g, i: (along_z(g), i), lambda b: b)
    banded_flow(vza_ref, lambda g, i: (along_z(i), g), lambda b: b)
    banded_flow(vzb_ref, lambda g, i: (along_z(i), g), lambda b: b + past)
    banded_flow(vxe_ref, lambda g, i: (i, g), lambda b: jnp.where(b < EDGE, b, b + middle))
    banded_flow(vye_ref, lambda g, i: (along_z(g), i), lambda b: jnp.where(b < EDGE, b, b + middle))
    cols = vf_ref.shape[1]
    plain = matmul(flow[...], short)
    for k in range(2):
        band = iota((half, cols), 1) // c - iota((half, cols), 0)
        vf_ref[k * half : (k + 1) * half] = jnp.where(band == 0, plain[k : k + 1, :cols], 0.0).astype(BF16)


def shift_right(value):
    return jnp.where(iota(value.shape, 1) == 0, jnp.zeros_like(value), pltpu.roll(value, 1, 1))


def shift_left(value):
    last = value.shape[1] - 1
    return jnp.where(iota(value.shape, 1) == last, jnp.zeros_like(value), pltpu.roll(value, last, 1))


def valid_sides():
    part_z = odd("gz")
    low = (lax.axis_index("gz") > 0).astype(F32)
    high = (lax.axis_index("gz") < lax.axis_size("gz") - 1).astype(F32)
    near = jnp.where(part_z == 1, low, high)
    far = jnp.where(part_z == 1, high, low)
    low_y = (lax.axis_index("gy") > 0).astype(F32)
    high_y = (lax.axis_index("gy") < lax.axis_size("gy") - 1).astype(F32)
    return near, far, low_y, high_y


def y_halos(rows, low_y, high_y):
    part_y = odd("gy")
    valid_even = jnp.where(part_y == 1, low_y, high_y)
    valid_odd = jnp.where(part_y == 1, high_y, low_y)
    return ((1 - part_y) * (rows + HALO), valid_even), (part_y * (rows + HALO), valid_odd)


def normalized(value, s1, t1, valid):
    count, c, cols = value.shape
    size = count * c
    value = jnp.maximum(value.reshape(size, cols).astype(F32) * s1[:size] + t1[:size], 0.0)
    if valid is not None:
        value = value * valid
    value = value.astype(BF16)
    return [v.reshape(count, c, cols) for v in (shift_right(value), value, shift_left(value))]


def set_masks(sm, tm, s2, t2, low_y, high_y):
    size, cols = s2.shape
    c = size // SPAN
    row = iota((size, cols), 0)
    for n, keep in enumerate((row >= 2 * c, row < size - 2 * c)):
        keep = jnp.where(keep, 1.0, high_y if n else low_y)
        sm[n] = s2[...] * keep
        tm[n] = t2[...] * keep


def activate(hidden, scale, shift, c, valid=None):
    value = jnp.maximum(hidden * scale + shift, 0.0)
    if valid is not None:
        value = value * valid
    return value.astype(BF16).reshape(-1, c, value.shape[1])


def stack(pieces):
    return jnp.concatenate([p.reshape(-1, p.shape[-1]) for p in pieces], axis=0)


def two_parts(value):
    half = value.shape[0] // 2
    return value[:half] + value[half:]


def along_x(value):
    value = two_parts(value)
    step = value.shape[0] // 3
    return shift_right(value[:step]) + value[step : 2 * step] + shift_left(value[2 * step :])


def edge_scale(s2, count, first, valid):
    c = s2.shape[0] // SPAN
    row = iota((count * c, s2.shape[1]), 0)
    keep = (row >= first * c) if first > 0 else (row < (count + first) * c)
    return jnp.where(keep, 1.0, valid)


def yz_parts(weights, cells):
    value = two_parts(matmul(weights[...], cells))
    step = value.shape[0] // 3
    return [value[i * step : (i + 1) * step] for i in range(3)]


def layer_parts(layer, flow_xz, flow_xy, flow_yz, base, height):
    parts = [0.5 * flow_xz[0], None, 0.5 * flow_xz[1]]

    def plus(k, value):
        parts[k] = value if parts[k] is None else parts[k] + value

    for i in range(3):
        if layer + i - 1 in flow_yz:
            piece = 0.5 * flow_yz[layer + i - 1][i]
            plus(0, piece[:height])
            plus(1, piece[height:])
    if layer in flow_xy:
        piece = 0.5 * flow_xy[layer]
        plus(1, piece[:height])
        plus(2, piece[height:])
    if base is not None:
        plus(0, base[:height])
        plus(1, 0.5 * (base[:height] + base[height:]))
        plus(2, base[height:])
    return parts


def rim_kernel(
    own, yeven, yodd, wye, wzb, vye, vza, s1, t1, s2, t2, near_ref, corner_ref, unit, part,
):
    depth, rows, c, cols = own.shape
    for layer in range(HALO):
        near_ref[layer, :rows] = own[layer]
        near_ref[layer, rows : rows + HALO] = yeven[layer]
        near_ref[layer, rows + HALO :] = yodd[layer]
    for layer in range(2):
        for row in range(HALO):
            corner_ref[layer * 2 * HALO + row] = yeven[depth - 1 - layer, row]
            corner_ref[layer * 2 * HALO + HALO + row] = yodd[depth - 1 - layer, row]

    _, _, low_y, high_y = valid_sides()
    (at_even, valid_even), (at_odd, valid_odd) = y_halos(rows, low_y, high_y)

    def place(value, z, y, valid):
        for j, moved in enumerate(normalized(value, s1, t1, valid)):
            unit[j, z, pl.ds(y, value.shape[0])] = moved

    for z in range(3):
        layer = depth - 3 + z
        place(own[layer, :2], z, HALO, None)
        place(own[layer, rows - 2 :], z, HALO + rows - 2, None)
        place(yeven[layer], z, at_even, valid_even)
        place(yodd[layer], z, at_odd, valid_odd)
    keeps = (edge_scale(s2, EDGE, 2, low_y), edge_scale(s2, EDGE, -2, high_y))
    cells = []
    for keep, window in zip(keeps, (range(EDGE + 2), range(rows + 1, rows + 6))):
        data = stack([unit[1, i, y] for i in range(3) for y in window])
        cells.append(activate(matmul(wye[...], data), s2[: EDGE * c] * keep, t2[: EDGE * c] * keep, c))
    none = jnp.zeros((2 * c, cols), BF16)
    ends = []
    for at in (0, rows + 1):
        data = stack([p for j in range(3) for p in (none, *(unit[j, z, at + 2] for z in range(3)))])
        ends.append(activate(matmul(wzb[...], data)[2 * c :], s2[:c], t2[:c], c))
    flow = yz_parts(vye, stack(cells))[0]
    ends = [along_x(matmul(vza[...], stack([none, none, cell]))) for cell in ends]
    height = part.shape[1]
    part[0] = 0.5 * flow[:height]
    part[1] = 0.5 * flow[height:]
    part[2] = jnp.zeros((height, cols), F32)
    for at, flow in zip((0, rows + 1), ends):
        step = flow.shape[0] // 2
        part[0, at : at + 1] = part[0, at : at + 1] + 0.5 * flow[depth : depth + 1]
        part[2, at : at + 1] = 0.5 * flow[step + depth : step + depth + 1]
    for k in range(3):
        value = part[k]
        top = value.astype(BF16)
        corner_ref[4 * HALO + k, :height] = top
        corner_ref[4 * HALO + k, height:] = (value - top.astype(F32)).astype(BF16)


def near_kernel(
    own, near, yeven, yodd, wxy, wyz, wza, vxy, vyz, vza, vf, s1, t1, s2, t2, const,
    mean, tail, unit, feat, act_xy, act_yz, act_xz, sm, tm, fxz,
):
    depth, rows, c, cols = own.shape
    valid_near, _, low_y, high_y = valid_sides()
    (at_even, valid_even), (at_odd, valid_odd) = y_halos(rows, low_y, high_y)
    start = HALO + depth
    first = start - 2

    def place(value, z, y, valid):
        count = value.shape[0]
        if z >= HALO - 1:
            feat[z - HALO + 1, pl.ds(y, count)] = value
        for j, moved in enumerate(normalized(value, s1, t1, valid)):
            if z < first:
                unit[j, z, pl.ds(y, count)] = moved
            else:
                tail[j, z - first, pl.ds(y, count)] = moved

    for z in range(depth):
        place(own[z], HALO + z, HALO, None)
        place(yeven[z], HALO + z, at_even, valid_even)
        place(yodd[z], HALO + z, at_odd, valid_odd)
    for z in range(HALO):
        place(near[z, :rows], HALO - 1 - z, HALO, valid_near)
        place(near[z, rows : rows + HALO], HALO - 1 - z, at_even, valid_near * valid_even)
        place(near[z, rows + HALO :], HALO - 1 - z, at_odd, valid_near * valid_odd)
    set_masks(sm, tm, s2, t2, low_y, high_y)

    def read(j, z, y):
        return unit[j, z, y] if z < first else tail[j, z - first, y]

    wide = rows + 4
    for n, z in enumerate(range(2, start)):
        for w in range(wide // SPAN):
            data = stack([read(j, z, slice(w * SPAN, w * SPAN + WIDE)) for j in range(3)])
            act_xy[n, w * SPAN : (w + 1) * SPAN] = activate(matmul(wxy[...], data), sm[w], tm[w], c)
    for n, z in enumerate(range(1, first + 1)):
        valid = valid_near if z < HALO else None
        for w in range(wide // SPAN):
            data = stack([read(1, z + i - 1, slice(w * SPAN, w * SPAN + WIDE)) for i in range(3)])
            act_yz[n, w * SPAN : (w + 1) * SPAN] = activate(matmul(wyz[...], data), sm[w], tm[w], c, valid)
    count = depth + 1
    keep = edge_scale(s2, count, 2, valid_near)
    scale, shift = s2[: count * c] * keep, t2[: count * c] * keep
    for y in range(rows + 2):
        data = stack([read(j, z, y + 2) for j in range(3) for z in range(depth + 3)])
        act_xz[y] = activate(matmul(wza[...], data), scale, shift, c)
    for y in range(rows + 2):
        flow = along_x(matmul(vza[...], act_xz[y].reshape(-1, cols)))
        half = flow.shape[0] // 2
        for k in range(2):
            fxz[k, :, y, :] = flow[k * half : (k + 1) * half]
    height = mean.shape[2]
    flow_xy = {z: along_x(matmul(vxy[...], act_xy[n].reshape(-1, cols))) for n, z in enumerate(range(2, start))}
    flow_yz = {z: yz_parts(vyz, act_yz[n].reshape(-1, cols)) for n, z in enumerate(range(1, first + 1))}
    for layer in range(2, start):
        at = layer - 2
        base = matmul(vf[...], feat[at, 2 : rows + 4].reshape(-1, cols)) + const[...]
        for k, value in enumerate(layer_parts(layer, (fxz[0, at], fxz[1, at]), flow_xy, flow_yz, base, height)):
            mean[k, at] = value


def mid_kernel(
    last, far, tail, wxy, wyz, wzb, vxy, vyz, vzb, vf, s1, t1, s2, t2, const,
    more, face, fxz,
):
    _, rows, c, cols = far.shape
    _, valid_far, _, _ = valid_sides()
    for z in range(HALO):
        for j, moved in enumerate(normalized(far[z], s1, t1, valid_far)):
            face[j, z] = moved

    def read(j, z, y):
        return tail[j, z, y + HALO] if z < 2 else face[j, z - 2, y]

    keep = edge_scale(s2, EDGE, -2, valid_far)
    scale, shift = s2[: EDGE * c] * keep, t2[: EDGE * c] * keep
    gap = jnp.zeros((EDGE * c, cols), BF16)

    def middle(cells):
        return jnp.concatenate([gap, cells.reshape(-1, cols), gap], axis=0)

    inner = slice(HALO, HALO + rows)
    data = stack([face[j, 0] for j in range(3)])
    act_xy = activate(matmul(wxy[...], data), s2[...], t2[...], c)
    act_yz = []
    for z in range(1, 4):
        data = stack([tail[1, i, inner] if i < 2 else face[1, i - 2] for i in range(z - 1, z + 2)])
        act_yz.append(activate(matmul(wyz[...], data), s2[...], t2[...], c, valid_far if z > 1 else None))
    act_xz = []
    for y in range(rows):
        data = stack([read(j, z, y) for j in range(3) for z in range(EDGE + 2)])
        act_xz.append(activate(matmul(wzb[...], data), scale, shift, c))
    flow_xy = {2: along_x(matmul(vxy[...], middle(act_xy)))}
    flow_yz = {z: yz_parts(vyz, middle(act_yz[z - 1])) for z in range(1, 4)}
    flow_xz = [along_x(matmul(vzb[...], cells.reshape(-1, cols))) for cells in act_xz]
    fxz[...] = jnp.zeros_like(fxz)
    for y, flow in enumerate(flow_xz):
        half = flow.shape[0] // 2
        for k in range(2):
            fxz[k, :, y + 1, :] = flow[k * half : (k + 1) * half]
    height = more.shape[2]
    for layer in range(3):
        base = None
        if layer == 2:
            cells = jnp.concatenate([gap[:c], far[0].reshape(-1, cols), gap[:c]], axis=0)
            base = matmul(vf[...], cells) + const[...]
        at = last + layer - 2
        for k, value in enumerate(layer_parts(layer, (fxz[0, at], fxz[1, at]), flow_xy, flow_yz, base, height)):
            more[k, layer] = value


def far_kernel(
    corner, tail, face, mean, more, wzb, wxe, wye, vzb, vxe, vye, vf, s1, t1, s2, t2,
    out, unit, fxz, feat, total,
):
    _, depth, rows, cols = out.shape
    c = corner.shape[1]
    valid_near, valid_far, low_y, high_y = valid_sides()
    (at_even, valid_even), (at_odd, valid_odd) = y_halos(rows, low_y, high_y)
    start = HALO + depth
    first = start - 2

    def place(value, z, y, valid):
        count = value.shape[0]
        if z == 0:
            feat[pl.ds(y, count)] = value
        for j, moved in enumerate(normalized(value, s1, t1, valid)):
            unit[j, z, pl.ds(y, count)] = moved

    for z in range(2):
        at = z * 2 * HALO
        place(corner[at : at + HALO], z, at_even, valid_far * valid_even)
        place(corner[at + HALO : at + 2 * HALO], z, at_odd, valid_far * valid_odd)

    def read(j, z, y):
        if z < start:
            return tail[j, z - first, y]
        return face[j, z - start, y - HALO] if HALO <= y < HALO + rows else unit[j, z - start, y]

    low, high = range(EDGE + 2), range(rows + 1, rows + 6)
    keeps = (edge_scale(s2, EDGE, 2, low_y), edge_scale(s2, EDGE, -2, high_y))
    scales = [s2[: EDGE * c] * keep for keep in keeps]
    shifts = [t2[: EDGE * c] * keep for keep in keeps]
    keep = edge_scale(s2, 2, -1, valid_far)
    scale, shift = s2[: 2 * c] * keep, t2[: 2 * c] * keep
    none = jnp.zeros((c, cols), BF16)
    act_xy = []
    for side, window in enumerate((low, high)):
        data = stack([read(j, start, y) for j in range(3) for y in window])
        act_xy.append(activate(matmul(wxe[...], data), scales[side], shifts[side], c))
    act_yz = {}
    for z in range(first + 1, start + 1):
        for side, window in enumerate((low, high)):
            data = stack([read(1, z + i - 1, y) for i in range(3) for y in window])
            valid = valid_far if z >= start else None
            act_yz[z, side] = activate(matmul(wye[...], data), scales[side], shifts[side], c, valid)
    act_xz = []
    for y in (0, rows + 1):
        data = stack([p for j in range(3) for p in (*(read(j, first + z, y + 2) for z in range(4)), none)])
        act_xz.append(activate(matmul(wzb[...], data)[: 2 * c], scale, shift, c))
    flow_xy = {start: along_x(matmul(vxe[...], stack(act_xy)))}
    flow_yz = {z: yz_parts(vye, stack([act_yz[z, 0], act_yz[z, 1]])) for z in range(first + 1, start + 1)}
    flow_xz = [along_x(matmul(vzb[...], stack([cells, none]))) for cells in act_xz]
    fxz[...] = jnp.zeros_like(fxz)
    for y, flow in zip((0, rows + 1), flow_xz):
        half = flow.shape[0] // 2
        for k in range(2):
            fxz[k, :, y, :] = flow[k * half : (k + 1) * half]
    gap = jnp.zeros((rows * c, cols), BF16)
    base = matmul(vf[...], jnp.concatenate([feat[2], gap, feat[rows + 3]], axis=0))

    height = mean.shape[2]
    spot = iota((height, cols), 0)
    inside_y = jnp.where(spot == 0, low_y, jnp.where(spot == rows + 1, high_y, jnp.where(spot < rows + 1, 1.0, 0.0)))
    for layer in range(2, start + 1):
        at = layer - 2
        keep = inside_y * valid_near if at == 0 else inside_y * valid_far if layer == start else inside_y
        if layer < first:
            for k in range(3):
                total[k, at] = mean[k, at] * keep
        else:
            added = layer_parts(
                layer, (fxz[0, at], fxz[1, at]), flow_xy, flow_yz, base if layer == start else None, height
            )
            for k in range(3):
                value = more[k, layer - first] + added[k]
                if layer < start:
                    value = value + mean[k, at]
                else:
                    value = value + corner[4 * HALO + k, :height].astype(F32) + corner[4 * HALO + k, height:].astype(F32)
                total[k, at] = value * keep
    part_z = odd("gz")
    for k in range(3):
        for z in range(depth):
            value = 0.25 * (total[k, z] + total[k, z + 2]) + 0.5 * total[k, z + 1]
            value = 0.25 * (value[:rows] + value[2 : rows + 2]) + 0.5 * value[1 : rows + 1]
            value = 0.25 * (shift_right(value) + shift_left(value)) + 0.5 * value
            out[k, part_z * z + (1 - part_z) * (depth - 1 - z)] = value


def shards(
    features, scale_first, shift_first, conv_first, bias_first,
    scale_second, shift_second, conv_second, bias_second, flow_weight,
):
    c, depth, rows, cols = features.shape
    shape = jax.ShapeDtypeStruct
    cells = functools.partial(shape, dtype=BF16)
    side = cells((depth, HALO, c, cols))
    own, send_even, send_odd, send_far = call(
        pack_kernel,
        [cells((depth, rows, c, cols)), side, side, cells((HALO, rows, c, cols))],
        [features], 2 * features.size * c * rows, 6,
    )
    yeven = swap(send_even, "gy", 0)
    yodd = swap(send_odd, "gy", 1)
    far = swap(send_far, "gz", 1)

    broad = rows + 2 * HALO
    high = -(-(rows + 2) // 8) * 8
    deep = -(-(depth + 2) // 8) * 8
    params = [
        scale_first[None], shift_first[None], conv_first, bias_first[None],
        scale_second[None], shift_second[None], conv_second, bias_second[None], flow_weight,
    ]
    params = [pltpu.with_memory_space_constraint(p, pltpu.HBM) for p in params]
    wxy, wyz, wza, wzb, wxe, wye, vxy, vyz, vza, vzb, vxe, vye, vf, *rest = call(
        weights_kernel,
        [
            cells((SPAN * c, 3 * WIDE * c)),
            cells((SPAN * c, 3 * WIDE * c)),
            cells(((depth + 1) * c, 3 * (depth + 3) * c)),
            *[cells((EDGE * c, 3 * (EDGE + 2) * c))] * 3,
            cells((12 * high, (rows + 4) * c)),
            cells((12 * high, (rows + 4) * c)),
            cells((12 * deep, (depth + 1) * c)),
            cells((12 * deep, EDGE * c)),
            *[cells((12 * high, 2 * EDGE * c))] * 2,
            cells((2 * high, (rows + 2) * c)),
            shape((rows * c, cols), F32),
            shape((rows * c, cols), F32),
            shape((SPAN * c, cols), F32),
            shape((SPAN * c, cols), F32),
            shape((2 * high, cols), F32),
        ],
        params,
        2 * 10**9, 10,
        [
            *(pltpu.VMEM(p.shape, p.dtype) for p in params),
            pltpu.VMEM((3, 3, c, 3 * WIDE * c), F32),
            pltpu.VMEM((3, 3, 2, 2, (rows + 4) * c), F32),
            pltpu.SemaphoreType.DMA((len(params),)),
        ],
        HBM,
    )
    assert c == 2 * high
    send_near, send_corner = call(
        rim_kernel,
        [cells((HALO, broad, c, cols)), cells((4 * HALO + 3, c, cols))],
        [own, yeven, yodd, wye, wzb, vye, vza, *rest[:4]],
        10**8, 10,
        [pltpu.VMEM((3, 3, broad, c, cols), BF16), pltpu.VMEM((3, high, cols), F32)],
    )
    corner = swap(send_corner, "gz", 1)
    near = swap(send_near, "gz", 0)

    mean, tail = call(
        near_kernel,
        [shape((3, depth + 1, high, cols), F32), cells((3, 2, broad, c, cols))],
        [own, near, yeven, yodd, wxy, wyz, wza, vxy, vyz, vza, vf, *rest],
        6 * 10**9, 24,
        [
            pltpu.VMEM((3, depth + 1, broad, c, cols), BF16),
            pltpu.VMEM((depth + 1, broad, c, cols), BF16),
            pltpu.VMEM((depth + 1, rows + 4, c, cols), BF16),
            pltpu.VMEM((depth + 1, rows + 4, c, cols), BF16),
            pltpu.VMEM((rows + 2, depth + 1, c, cols), BF16),
            pltpu.VMEM((2, SPAN * c, cols), F32),
            pltpu.VMEM((2, SPAN * c, cols), F32),
            pltpu.VMEM((2, deep, high, cols), F32),
        ],
    )
    more, face = call(
        functools.partial(mid_kernel, depth + 1),
        [shape((3, 3, high, cols), F32), cells((3, HALO, rows, c, cols))],
        [far, tail, wxy, wyz, wzb, vxy, vyz, vzb, vf, *rest],
        3 * 10**9, 12,
        [pltpu.VMEM((2, deep, high, cols), F32)],
    )
    (out,) = call(
        far_kernel,
        [shape((3, depth, rows, cols), F32)],
        [corner, tail, face, mean, more, wzb, wxe, wye, vzb, vxe, vye, vf, *rest[:4]],
        2 * 10**9, 16,
        [
            pltpu.VMEM((3, HALO, broad, c, cols), BF16),
            pltpu.VMEM((2, deep, high, cols), F32),
            pltpu.VMEM((broad, c, cols), BF16),
            pltpu.VMEM((3, depth + 2, high, cols), F32),
        ],
    )
    return out


def solution(mesh):
    return jax.shard_map(
        shards,
        mesh=mesh,
        in_specs=(P(None, "gz", "gy", None), P(), P(), P(), P(), P(), P(), P(), P(), P()),
        out_specs=P(None, "gz", "gy", None),
        check_vma=False,
    )
```

```python
import functools

import jax
import jax.numpy as jnp
from jax import lax
from jax.experimental import pallas as pl
from jax.experimental.pallas import tpu as pltpu
from jax.sharding import PartitionSpec as P


HALO = 3
SPAN = 6
WIDE = SPAN + 2
EDGE = 3
F32, BF16 = jnp.float32, jnp.bfloat16
VMEM = pl.BlockSpec(memory_space=pltpu.VMEM)
HBM = pl.BlockSpec(memory_space=pltpu.HBM)


def iota(shape, dim):
    return lax.broadcasted_iota(jnp.int32, shape, dim)


def matmul(a, b):
    return jnp.dot(a, b, preferred_element_type=F32)


def swap(value, axis, first):
    pairs = []
    for i in range(first, lax.axis_size(axis) - 1, 2):
        pairs += [(i, i + 1), (i + 1, i)]
    return lax.ppermute(value, axis, pairs)


def call(kernel, outs, args, flops, mib, scratch=(), space=VMEM):
    nbytes = sum(a.size * a.dtype.itemsize for a in (*outs, *args))
    return pl.pallas_call(
        kernel,
        out_shape=outs,
        in_specs=[space] * len(args),
        out_specs=[VMEM] * len(outs),
        scratch_shapes=list(scratch),
        cost_estimate=pl.CostEstimate(flops=flops, bytes_accessed=nbytes, transcendentals=0),
        compiler_params=pltpu.CompilerParams(vmem_limit_bytes=mib * 2**20),
    )(*args)


def odd(axis):
    return lax.rem(lax.axis_index(axis), 2)


def cell_order(channels, rows):
    size = channels * rows
    row, col = iota((size, size), 0), iota((size, size), 1)
    return ((row // channels == col % rows) & (row % channels == col // rows)).astype(F32).astype(BF16)


def pack_kernel(feat_hbm, *refs):
    count = (len(refs) - 6) // 2
    own_ref, even_ref, odd_ref, far_ref = refs[count : count + 4]
    feat_ref, sem = refs[-2:]
    copies = [pltpu.make_async_copy(feat_hbm, feat_ref, sem.at[count])]
    for n in range(count):
        copies.append(pltpu.make_async_copy(refs[n], refs[count + 4 + n], sem.at[n]))
    for copy in copies:
        copy.start()
    channels, depth, rows, cols = feat_ref.shape
    size = channels * rows
    order = cell_order(channels, rows)
    part_z, part_y = odd("gz"), odd("gy")
    copies[0].wait()
    for z in range(depth):
        value = feat_ref[:, z].astype(F32).reshape(size, cols).astype(BF16)
        value = matmul(order, value).astype(BF16).reshape(rows, channels, cols)
        own_ref[part_z * z + (1 - part_z) * (depth - 1 - z)] = value
    first_even, first_odd = (1 - part_y) * (rows - HALO), part_y * (rows - HALO)
    for z in range(depth):
        for row in range(HALO):
            even_ref[z, row] = own_ref[z, first_even + row]
            odd_ref[z, row] = own_ref[z, first_odd + row]
    for layer in range(2):
        far_ref[layer] = own_ref[depth - 1 - layer]
    for copy in copies[1:]:
        copy.wait()


def weights_kernel(
    scale1, shift1, conv1, bias1, scale2, shift2, conv2, bias2, flow,
    wxy_ref, wyz_ref, wza_ref, wzb_ref, wxe_ref, wye_ref, wzc_ref,
    vxy_ref, vyz_ref, vza_ref, vzb_ref, vxe_ref, vye_ref, vzc_ref, vf_ref,
    s1_ref, t1_ref, s2_ref, t2_ref, const_ref,
    taps, folds,
):
    c = conv1.shape[-1]
    part_z = odd("gz")

    def along_z(i):
        return part_z * i + (1 - part_z) * (2 - i)

    def spread(vector, rows, cols):
        pick = iota((rows, c), 0) % c == iota((rows, c), 1)
        column = jnp.sum(jnp.where(pick, vector, 0.0), axis=1, keepdims=True)
        return jnp.broadcast_to(column, (rows, cols))

    s1_ref[...] = spread(scale1[...], *s1_ref.shape)
    t1_ref[...] = spread(shift1[...], *t1_ref.shape)
    s2_ref[...] = spread(scale2[...], *s2_ref.shape)
    t2_ref[...] = spread(bias1[...] * scale2[...] + shift2[...], *t2_ref.shape)
    const = jnp.sum(flow[...].astype(F32) * bias2[...], axis=1, keepdims=True)
    half = const_ref.shape[0] // 2
    for k in range(2):
        const_ref[k * half : (k + 1) * half] = jnp.broadcast_to(const[k : k + 1], (half, const_ref.shape[1]))

    def tile_of(cols):
        return (iota((c, cols), 0) == iota((c, cols), 1) % c).astype(F32).astype(BF16)

    tile = tile_of(taps.shape[-1])
    short = tile_of(folds.shape[-1])
    for i in range(3):
        for j in range(3):
            taps[i, j] = matmul(conv1[i, j], tile)
            both = matmul(flow[...], conv2[i, j])
            high = both.astype(BF16)
            low = (both - high.astype(F32)).astype(BF16)
            folds[i, j, 0] = matmul(high, short)
            folds[i, j, 1] = matmul(low, short)

    def banded(ref, pick):
        rows, cols = ref.shape
        group = cols // 3
        lane = iota((c, cols), 1)
        slot = lane % group // c
        for a in range(rows // c):
            value = jnp.zeros((c, cols), F32)
            for g in range(3):
                for i in range(3):
                    value = jnp.where((slot == a + i) & (lane // group == g), pick(g, i)[:, :cols], value)
            ref[a * c : (a + 1) * c] = value.astype(BF16)

    banded(wxy_ref, lambda g, i: taps[i, g])
    banded(wyz_ref, lambda g, i: taps[along_z(g), i])
    banded(wza_ref, lambda g, i: taps[along_z(i), g])
    banded(wzb_ref, lambda g, i: taps[along_z(i), g])
    banded(wxe_ref, lambda g, i: taps[i, g])
    banded(wye_ref, lambda g, i: taps[along_z(g), i])
    banded(wzc_ref, lambda g, i: taps[along_z(i), g])

    def banded_flow(ref, pick, place, steps=3):
        cols = ref.shape[1]
        height = ref.shape[0] // 12
        band = place(iota((height, cols), 1) // c) - iota((height, cols), 0)
        for part in range(2):
            for g in range(3):
                for k in range(2):
                    block = jnp.zeros((height, cols), F32)
                    for i in range(steps):
                        row, col = pick(g, i)
                        block = jnp.where(band == i, folds[row, col, part, k : k + 1, :cols], block)
                    at = ((part * 3 + g) * 2 + k) * height
                    ref[at : at + height] = block.astype(BF16)

    middle = vxy_ref.shape[1] // c - 2 * EDGE
    past = vza_ref.shape[1] // c
    banded_flow(vxy_ref, lambda g, i: (i, g), lambda b: b)
    banded_flow(vyz_ref, lambda g, i: (along_z(g), i), lambda b: b)
    banded_flow(vza_ref, lambda g, i: (along_z(i), g), lambda b: b)
    banded_flow(vzb_ref, lambda g, i: (along_z(i), g), lambda b: b + past)
    banded_flow(vxe_ref, lambda g, i: (i, g), lambda b: jnp.where(b < EDGE, b, b + middle))
    banded_flow(vye_ref, lambda g, i: (along_z(g), i), lambda b: jnp.where(b < EDGE, b, b + middle))
    banded_flow(vzc_ref, lambda g, i: (along_z(i), g), lambda b: b, 1)
    cols = vf_ref.shape[1]
    plain = matmul(flow[...], short)
    for k in range(2):
        band = iota((half, cols), 1) // c - iota((half, cols), 0)
        vf_ref[k * half : (k + 1) * half] = jnp.where(band == 0, plain[k : k + 1, :cols], 0.0).astype(BF16)


def shift_right(value):
    return jnp.where(iota(value.shape, 1) == 0, jnp.zeros_like(value), pltpu.roll(value, 1, 1))


def shift_left(value):
    last = value.shape[1] - 1
    return jnp.where(iota(value.shape, 1) == last, jnp.zeros_like(value), pltpu.roll(value, last, 1))


def valid_sides():
    part_z = odd("gz")
    low = (lax.axis_index("gz") > 0).astype(F32)
    high = (lax.axis_index("gz") < lax.axis_size("gz") - 1).astype(F32)
    near = jnp.where(part_z == 1, low, high)
    far = jnp.where(part_z == 1, high, low)
    low_y = (lax.axis_index("gy") > 0).astype(F32)
    high_y = (lax.axis_index("gy") < lax.axis_size("gy") - 1).astype(F32)
    return near, far, low_y, high_y


def y_halos(rows, low_y, high_y):
    part_y = odd("gy")
    valid_even = jnp.where(part_y == 1, low_y, high_y)
    valid_odd = jnp.where(part_y == 1, high_y, low_y)
    return ((1 - part_y) * (rows + HALO), valid_even), (part_y * (rows + HALO), valid_odd)


def normalized(value, s1, t1, valid):
    count, c, cols = value.shape
    size = count * c
    value = jnp.maximum(value.reshape(size, cols).astype(F32) * s1[:size] + t1[:size], 0.0)
    if valid is not None:
        value = value * valid
    value = value.astype(BF16)
    return [v.reshape(count, c, cols) for v in (shift_right(value), value, shift_left(value))]


def set_masks(sm, tm, s2, t2, low_y, high_y):
    size, cols = s2.shape
    c = size // SPAN
    row = iota((size, cols), 0)
    for n, keep in enumerate((row >= 2 * c, row < size - 2 * c)):
        keep = jnp.where(keep, 1.0, high_y if n else low_y)
        sm[n] = s2[...] * keep
        tm[n] = t2[...] * keep


def activate(hidden, scale, shift, c, valid=None):
    value = jnp.maximum(hidden * scale + shift, 0.0)
    if valid is not None:
        value = value * valid
    return value.astype(BF16).reshape(-1, c, value.shape[1])


def stack(pieces):
    return jnp.concatenate([p.reshape(-1, p.shape[-1]) for p in pieces], axis=0)


def two_parts(value):
    half = value.shape[0] // 2
    return value[:half] + value[half:]


def along_x(value):
    value = two_parts(value)
    step = value.shape[0] // 3
    return shift_right(value[:step]) + value[step : 2 * step] + shift_left(value[2 * step :])


def edge_scale(s2, count, first, valid):
    c = s2.shape[0] // SPAN
    row = iota((count * c, s2.shape[1]), 0)
    keep = (row >= first * c) if first > 0 else (row < (count + first) * c)
    return jnp.where(keep, 1.0, valid)


def yz_parts(weights, cells):
    value = two_parts(matmul(weights[...], cells))
    step = value.shape[0] // 3
    return [value[i * step : (i + 1) * step] for i in range(3)]


def layer_parts(layer, flow_xz, flow_xy, flow_yz, base, height):
    parts = [0.5 * flow_xz[0], None, 0.5 * flow_xz[1]]

    def plus(k, value):
        parts[k] = value if parts[k] is None else parts[k] + value

    for i in range(3):
        if layer + i - 1 in flow_yz:
            piece = 0.5 * flow_yz[layer + i - 1][i]
            plus(0, piece[:height])
            plus(1, piece[height:])
    if layer in flow_xy:
        piece = 0.5 * flow_xy[layer]
        plus(1, piece[:height])
        plus(2, piece[height:])
    if base is not None:
        plus(0, base[:height])
        plus(1, 0.5 * (base[:height] + base[height:]))
        plus(2, base[height:])
    return parts


def rim_kernel(
    own, yeven, yodd, wyz, wzc, vyz, vzc, s1, t1, s2, t2, near_ref, corner_ref, unit,
):
    depth, rows, c, _ = own.shape
    for layer in range(HALO):
        near_ref[layer, :rows] = own[layer]
        near_ref[layer, rows : rows + HALO] = yeven[layer]
        near_ref[layer, rows + HALO :] = yodd[layer]
    for layer in range(2):
        for row in range(HALO):
            corner_ref[layer * 2 * HALO + row] = yeven[depth - 1 - layer, row]
            corner_ref[layer * 2 * HALO + HALO + row] = yodd[depth - 1 - layer, row]

    _, _, low_y, high_y = valid_sides()
    (at_even, valid_even), (at_odd, valid_odd) = y_halos(rows, low_y, high_y)

    def place(value, z, y, valid):
        for j, moved in enumerate(normalized(value, s1, t1, valid)):
            unit[j, z, pl.ds(y, value.shape[0])] = moved

    for z in range(3):
        layer = depth - 3 + z
        place(own[layer], z, HALO, None)
        place(yeven[layer], z, at_even, valid_even)
        place(yodd[layer], z, at_odd, valid_odd)
    keeps = (edge_scale(s2, SPAN, 2, low_y), edge_scale(s2, SPAN, -2, high_y))
    act_yz = []
    for w, keep in enumerate(keeps):
        data = stack([unit[1, i, w * SPAN : w * SPAN + WIDE] for i in range(3)])
        act_yz.append(activate(matmul(wyz[...], data), s2[...] * keep, t2[...] * keep, c))
    act_xz = []
    for y in range(rows + 2):
        data = stack([unit[j, z, y + 2] for j in range(3) for z in range(3)])
        act_xz.append(activate(matmul(wzc[...], data), s2[:c], t2[:c], c))
    flow_yz = 0.5 * yz_parts(vyz, stack(act_yz))[0]
    flow_xz = 0.5 * along_x(matmul(vzc[...], stack(act_xz)))
    height = flow_xz.shape[0] // 2
    for k, value in enumerate((flow_yz[:height] + flow_xz[:height], flow_yz[height:], flow_xz[height:])):
        top = value.astype(BF16)
        corner_ref[4 * HALO + k, :height] = top
        corner_ref[4 * HALO + k, height:] = (value - top.astype(F32)).astype(BF16)


def near_kernel(
    own, near, yeven, yodd, wxy, wyz, wza, vxy, vyz, vza, vf, s1, t1, s2, t2, const,
    mean, tail, unit, feat, act_xy, act_yz, act_xz, sm, tm, fxz,
):
    depth, rows, c, cols = own.shape
    valid_near, _, low_y, high_y = valid_sides()
    (at_even, valid_even), (at_odd, valid_odd) = y_halos(rows, low_y, high_y)
    start = HALO + depth
    first = start - 2

    def place(value, z, y, valid):
        count = value.shape[0]
        if z >= HALO - 1:
            feat[z - HALO + 1, pl.ds(y, count)] = value
        for j, moved in enumerate(normalized(value, s1, t1, valid)):
            if z < first:
                unit[j, z, pl.ds(y, count)] = moved
            else:
                tail[j, z - first, pl.ds(y, count)] = moved

    for z in range(depth):
        place(own[z], HALO + z, HALO, None)
        place(yeven[z], HALO + z, at_even, valid_even)
        place(yodd[z], HALO + z, at_odd, valid_odd)
    for z in range(HALO):
        place(near[z, :rows], HALO - 1 - z, HALO, valid_near)
        place(near[z, rows : rows + HALO], HALO - 1 - z, at_even, valid_near * valid_even)
        place(near[z, rows + HALO :], HALO - 1 - z, at_odd, valid_near * valid_odd)
    set_masks(sm, tm, s2, t2, low_y, high_y)

    def read(j, z, y):
        return unit[j, z, y] if z < first else tail[j, z - first, y]

    wide = rows + 4
    for n, z in enumerate(range(2, start)):
        for w in range(wide // SPAN):
            data = stack([read(j, z, slice(w * SPAN, w * SPAN + WIDE)) for j in range(3)])
            act_xy[n, w * SPAN : (w + 1) * SPAN] = activate(matmul(wxy[...], data), sm[w], tm[w], c)
    for n, z in enumerate(range(1, first + 1)):
        valid = valid_near if z < HALO else None
        for w in range(wide // SPAN):
            data = stack([read(1, z + i - 1, slice(w * SPAN, w * SPAN + WIDE)) for i in range(3)])
            act_yz[n, w * SPAN : (w + 1) * SPAN] = activate(matmul(wyz[...], data), sm[w], tm[w], c, valid)
    count = depth + 1
    keep = edge_scale(s2, count, 2, valid_near)
    scale, shift = s2[: count * c] * keep, t2[: count * c] * keep
    for y in range(rows + 2):
        data = stack([read(j, z, y + 2) for j in range(3) for z in range(depth + 3)])
        act_xz[y] = activate(matmul(wza[...], data), scale, shift, c)
    for y in range(rows + 2):
        flow = along_x(matmul(vza[...], act_xz[y].reshape(-1, cols)))
        half = flow.shape[0] // 2
        for k in range(2):
            fxz[k, :, y, :] = flow[k * half : (k + 1) * half]
    height = mean.shape[2]
    flow_xy = {z: along_x(matmul(vxy[...], act_xy[n].reshape(-1, cols))) for n, z in enumerate(range(2, start))}
    flow_yz = {z: yz_parts(vyz, act_yz[n].reshape(-1, cols)) for n, z in enumerate(range(1, first + 1))}
    for layer in range(2, start):
        at = layer - 2
        base = matmul(vf[...], feat[at, 2 : rows + 4].reshape(-1, cols)) + const[...]
        for k, value in enumerate(layer_parts(layer, (fxz[0, at], fxz[1, at]), flow_xy, flow_yz, base, height)):
            mean[k, at] = value


def mid_kernel(
    last, far, tail, wxy, wyz, wzb, vxy, vyz, vzb, vf, s1, t1, s2, t2, const,
    more, face, fxz,
):
    _, rows, c, cols = far.shape
    _, valid_far, _, _ = valid_sides()
    for z in range(2):
        for j, moved in enumerate(normalized(far[z], s1, t1, valid_far)):
            face[j, z] = moved

    def read(j, z, y):
        return tail[j, z, y + HALO] if z < 2 else face[j, z - 2, y]

    keep = edge_scale(s2, 2, -1, valid_far)
    scale, shift = s2[: 2 * c] * keep, t2[: 2 * c] * keep
    none = jnp.zeros((c, cols), BF16)
    gap = jnp.zeros((EDGE * c, cols), BF16)

    def middle(cells):
        return jnp.concatenate([gap, cells.reshape(-1, cols), gap], axis=0)

    inner = slice(HALO, HALO + rows)
    data = stack([face[j, 0] for j in range(3)])
    act_xy = activate(matmul(wxy[...], data), s2[...], t2[...], c)
    act_yz = []
    for z in range(1, 3):
        data = stack([tail[1, i, inner] if i < 2 else face[1, i - 2] for i in range(z - 1, z + 2)])
        act_yz.append(activate(matmul(wyz[...], data), s2[...], t2[...], c, valid_far if z > 1 else None))
    act_xz = []
    for y in range(rows):
        data = stack([p for j in range(3) for p in (*(read(j, z, y) for z in range(4)), none)])
        act_xz.append(activate(matmul(wzb[...], data)[: 2 * c], scale, shift, c))
    flow_xy = {2: along_x(matmul(vxy[...], middle(act_xy)))}
    flow_yz = {z: yz_parts(vyz, middle(act_yz[z - 1])) for z in range(1, 3)}
    flow_xz = [along_x(matmul(vzb[...], stack([cells, none]))) for cells in act_xz]
    fxz[...] = jnp.zeros_like(fxz)
    for y, flow in enumerate(flow_xz):
        half = flow.shape[0] // 2
        for k in range(2):
            fxz[k, :, y + 1, :] = flow[k * half : (k + 1) * half]
    height = more.shape[2]
    for layer in range(3):
        base = None
        if layer == 2:
            cells = jnp.concatenate([gap[:c], far[0].reshape(-1, cols), gap[:c]], axis=0)
            base = matmul(vf[...], cells) + const[...]
        at = last + layer - 2
        for k, value in enumerate(layer_parts(layer, (fxz[0, at], fxz[1, at]), flow_xy, flow_yz, base, height)):
            more[k, layer] = value


def far_kernel(
    corner, tail, face, mean, more, wzb, wxe, wye, vzb, vxe, vye, vf, s1, t1, s2, t2,
    out, unit, fxz, feat, total,
):
    _, depth, rows, cols = out.shape
    c = corner.shape[1]
    valid_near, valid_far, low_y, high_y = valid_sides()
    (at_even, valid_even), (at_odd, valid_odd) = y_halos(rows, low_y, high_y)
    start = HALO + depth
    first = start - 2

    def place(value, z, y, valid):
        count = value.shape[0]
        if z == 0:
            feat[pl.ds(y, count)] = value
        for j, moved in enumerate(normalized(value, s1, t1, valid)):
            unit[j, z, pl.ds(y, count)] = moved

    for z in range(2):
        at = z * 2 * HALO
        place(corner[at : at + HALO], z, at_even, valid_far * valid_even)
        place(corner[at + HALO : at + 2 * HALO], z, at_odd, valid_far * valid_odd)

    def read(j, z, y):
        if z < start:
            return tail[j, z - first, y]
        return face[j, z - start, y - HALO] if HALO <= y < HALO + rows else unit[j, z - start, y]

    low, high = range(EDGE + 2), range(rows + 1, rows + 6)
    keeps = (edge_scale(s2, EDGE, 2, low_y), edge_scale(s2, EDGE, -2, high_y))
    scales = [s2[: EDGE * c] * keep for keep in keeps]
    shifts = [t2[: EDGE * c] * keep for keep in keeps]
    keep = edge_scale(s2, 2, -1, valid_far)
    scale, shift = s2[: 2 * c] * keep, t2[: 2 * c] * keep
    none = jnp.zeros((c, cols), BF16)
    act_xy = []
    for side, window in enumerate((low, high)):
        data = stack([read(j, start, y) for j in range(3) for y in window])
        act_xy.append(activate(matmul(wxe[...], data), scales[side], shifts[side], c))
    act_yz = {}
    for z in range(first + 1, start + 1):
        for side, window in enumerate((low, high)):
            data = stack([read(1, z + i - 1, y) for i in range(3) for y in window])
            valid = valid_far if z >= start else None
            act_yz[z, side] = activate(matmul(wye[...], data), scales[side], shifts[side], c, valid)
    act_xz = []
    for y in (0, rows + 1):
        data = stack([p for j in range(3) for p in (*(read(j, first + z, y + 2) for z in range(4)), none)])
        act_xz.append(activate(matmul(wzb[...], data)[: 2 * c], scale, shift, c))
    flow_xy = {start: along_x(matmul(vxe[...], stack(act_xy)))}
    flow_yz = {z: yz_parts(vye, stack([act_yz[z, 0], act_yz[z, 1]])) for z in range(first + 1, start + 1)}
    flow_xz = [along_x(matmul(vzb[...], stack([cells, none]))) for cells in act_xz]
    fxz[...] = jnp.zeros_like(fxz)
    for y, flow in zip((0, rows + 1), flow_xz):
        half = flow.shape[0] // 2
        for k in range(2):
            fxz[k, :, y, :] = flow[k * half : (k + 1) * half]
    gap = jnp.zeros((rows * c, cols), BF16)
    base = matmul(vf[...], jnp.concatenate([feat[2], gap, feat[rows + 3]], axis=0))

    height = mean.shape[2]
    spot = iota((height, cols), 0)
    inside_y = jnp.where(spot == 0, low_y, jnp.where(spot == rows + 1, high_y, jnp.where(spot < rows + 1, 1.0, 0.0)))
    for layer in range(2, start + 1):
        at = layer - 2
        keep = inside_y * valid_near if at == 0 else inside_y * valid_far if layer == start else inside_y
        if layer < first:
            for k in range(3):
                total[k, at] = mean[k, at] * keep
        else:
            added = layer_parts(
                layer, (fxz[0, at], fxz[1, at]), flow_xy, flow_yz, base if layer == start else None, height
            )
            for k in range(3):
                value = more[k, layer - first] + added[k]
                if layer < start:
                    value = value + mean[k, at]
                else:
                    value = value + corner[4 * HALO + k, :height].astype(F32) + corner[4 * HALO + k, height:].astype(F32)
                total[k, at] = value * keep
    part_z = odd("gz")
    for k in range(3):
        for z in range(depth):
            value = 0.25 * (total[k, z] + total[k, z + 2]) + 0.5 * total[k, z + 1]
            value = 0.25 * (value[:rows] + value[2 : rows + 2]) + 0.5 * value[1 : rows + 1]
            value = 0.25 * (shift_right(value) + shift_left(value)) + 0.5 * value
            out[k, part_z * z + (1 - part_z) * (depth - 1 - z)] = value


def shards(
    features, scale_first, shift_first, conv_first, bias_first,
    scale_second, shift_second, conv_second, bias_second, flow_weight,
):
    c, depth, rows, cols = features.shape
    shape = jax.ShapeDtypeStruct
    cells = functools.partial(shape, dtype=BF16)
    side = cells((depth, HALO, c, cols))
    params = [
        scale_first[None], shift_first[None], conv_first, bias_first[None],
        scale_second[None], shift_second[None], conv_second, bias_second[None], flow_weight,
    ]
    params = [pltpu.with_memory_space_constraint(p, pltpu.HBM) for p in params]
    own, send_even, send_odd, send_far, *params = call(
        pack_kernel,
        [cells((depth, rows, c, cols)), side, side, cells((2, rows, c, cols))]
        + [shape(p.shape, p.dtype) for p in params],
        [pltpu.with_memory_space_constraint(features, pltpu.HBM), *params],
        2 * features.size * c * rows, 6,
        [pltpu.VMEM(features.shape, BF16), pltpu.SemaphoreType.DMA((len(params) + 1,))],
        HBM,
    )
    yeven = swap(send_even, "gy", 0)
    yodd = swap(send_odd, "gy", 1)
    far = swap(send_far, "gz", 1)

    broad = rows + 2 * HALO
    high = -(-(rows + 2) // 8) * 8
    deep = -(-(depth + 2) // 8) * 8
    wxy, wyz, wza, wzb, wxe, wye, wzc, vxy, vyz, vza, vzb, vxe, vye, vzc, vf, *rest = call(
        weights_kernel,
        [
            cells((SPAN * c, 3 * WIDE * c)),
            cells((SPAN * c, 3 * WIDE * c)),
            cells(((depth + 1) * c, 3 * (depth + 3) * c)),
            *[cells((EDGE * c, 3 * (EDGE + 2) * c))] * 3,
            cells((c, 9 * c)),
            cells((12 * high, (rows + 4) * c)),
            cells((12 * high, (rows + 4) * c)),
            cells((12 * deep, (depth + 1) * c)),
            cells((12 * deep, EDGE * c)),
            *[cells((12 * high, 2 * EDGE * c))] * 2,
            cells((12 * high, (rows + 2) * c)),
            cells((2 * high, (rows + 2) * c)),
            shape((rows * c, cols), F32),
            shape((rows * c, cols), F32),
            shape((SPAN * c, cols), F32),
            shape((SPAN * c, cols), F32),
            shape((2 * high, cols), F32),
        ],
        params,
        2 * 10**9, 10,
        [
            pltpu.VMEM((3, 3, c, 3 * WIDE * c), F32),
            pltpu.VMEM((3, 3, 2, 2, (rows + 4) * c), F32),
        ],
    )
    assert c == 2 * high
    send_near, send_corner = call(
        rim_kernel,
        [cells((HALO, broad, c, cols)), cells((4 * HALO + 3, c, cols))],
        [own, yeven, yodd, wyz, wzc, vyz, vzc, *rest[:4]],
        10**8, 10,
        [pltpu.VMEM((3, 3, broad, c, cols), BF16)],
    )
    corner = swap(send_corner, "gz", 1)
    near = swap(send_near, "gz", 0)

    mean, tail = call(
        near_kernel,
        [shape((3, depth + 1, high, cols), F32), cells((3, 2, broad, c, cols))],
        [own, near, yeven, yodd, wxy, wyz, wza, vxy, vyz, vza, vf, *rest],
        6 * 10**9, 24,
        [
            pltpu.VMEM((3, depth + 1, broad, c, cols), BF16),
            pltpu.VMEM((depth + 1, broad, c, cols), BF16),
            pltpu.VMEM((depth + 1, rows + 4, c, cols), BF16),
            pltpu.VMEM((depth + 1, rows + 4, c, cols), BF16),
            pltpu.VMEM((rows + 2, depth + 1, c, cols), BF16),
            pltpu.VMEM((2, SPAN * c, cols), F32),
            pltpu.VMEM((2, SPAN * c, cols), F32),
            pltpu.VMEM((2, deep, high, cols), F32),
        ],
    )
    more, face = call(
        functools.partial(mid_kernel, depth + 1),
        [shape((3, 3, high, cols), F32), cells((3, 2, rows, c, cols))],
        [far, tail, wxy, wyz, wzb, vxy, vyz, vzb, vf, *rest],
        3 * 10**9, 12,
        [pltpu.VMEM((2, deep, high, cols), F32)],
    )
    (out,) = call(
        far_kernel,
        [shape((3, depth, rows, cols), F32)],
        [corner, tail, face, mean, more, wzb, wxe, wye, vzb, vxe, vye, vf, *rest[:4]],
        2 * 10**9, 16,
        [
            pltpu.VMEM((3, HALO, broad, c, cols), BF16),
            pltpu.VMEM((2, deep, high, cols), F32),
            pltpu.VMEM((broad, c, cols), BF16),
            pltpu.VMEM((3, depth + 2, high, cols), F32),
        ],
    )
    return out


def solution(mesh):
    return jax.shard_map(
        shards,
        mesh=mesh,
        in_specs=(P(None, "gz", "gy", None), P(), P(), P(), P(), P(), P(), P(), P(), P()),
        out_specs=P(None, "gz", "gy", None),
        check_vma=False,
    )
```

```python
import functools

import jax
import jax.numpy as jnp
from jax import lax
from jax.experimental import pallas as pl
from jax.experimental.pallas import tpu as pltpu
from jax.sharding import PartitionSpec as P


HALO = 3
SPAN = 6
WIDE = SPAN + 2
EDGE = 3
F32, BF16 = jnp.float32, jnp.bfloat16
VMEM = pl.BlockSpec(memory_space=pltpu.VMEM)
HBM = pl.BlockSpec(memory_space=pltpu.HBM)


def iota(shape, dim):
    return lax.broadcasted_iota(jnp.int32, shape, dim)


def matmul(a, b):
    return jnp.dot(a, b, preferred_element_type=F32)


def swap(value, axis, first):
    pairs = []
    for i in range(first, lax.axis_size(axis) - 1, 2):
        pairs += [(i, i + 1), (i + 1, i)]
    return lax.ppermute(value, axis, pairs)


def call(kernel, outs, args, flops, mib, scratch=(), space=VMEM):
    nbytes = sum(a.size * a.dtype.itemsize for a in (*outs, *args))
    return pl.pallas_call(
        kernel,
        out_shape=outs,
        in_specs=[space] * len(args),
        out_specs=[VMEM] * len(outs),
        scratch_shapes=list(scratch),
        cost_estimate=pl.CostEstimate(flops=flops, bytes_accessed=nbytes, transcendentals=0),
        compiler_params=pltpu.CompilerParams(vmem_limit_bytes=mib * 2**20),
    )(*args)


def odd(axis):
    return lax.rem(lax.axis_index(axis), 2)


def cell_order(channels, rows):
    size = channels * rows
    row, col = iota((size, size), 0), iota((size, size), 1)
    return ((row // channels == col % rows) & (row % channels == col // rows)).astype(F32).astype(BF16)


def pack_kernel(feat_hbm, *refs):
    count = (len(refs) - 6) // 2
    own_ref, even_ref, odd_ref, far_ref = refs[count : count + 4]
    feat_ref, sem = refs[-2:]
    copies = [pltpu.make_async_copy(feat_hbm, feat_ref, sem.at[count])]
    for n in range(count):
        copies.append(pltpu.make_async_copy(refs[n], refs[count + 4 + n], sem.at[n]))
    for copy in copies:
        copy.start()
    channels, depth, rows, cols = feat_ref.shape
    size = channels * rows
    order = cell_order(channels, rows)
    part_z, part_y = odd("gz"), odd("gy")
    copies[0].wait()
    for z in range(depth):
        value = feat_ref[:, z].astype(F32).reshape(size, cols).astype(BF16)
        value = matmul(order, value).astype(BF16).reshape(rows, channels, cols)
        own_ref[part_z * z + (1 - part_z) * (depth - 1 - z)] = value
    first_even, first_odd = (1 - part_y) * (rows - HALO), part_y * (rows - HALO)
    for z in range(depth):
        for row in range(HALO):
            even_ref[z, row] = own_ref[z, first_even + row]
            odd_ref[z, row] = own_ref[z, first_odd + row]
    for layer in range(2):
        far_ref[layer] = own_ref[depth - 1 - layer]
    for copy in copies[1:]:
        copy.wait()


def weights_kernel(
    scale1, shift1, conv1, bias1, scale2, shift2, conv2, bias2, flow,
    wxy_ref, wyz_ref, wza_ref, wzb_ref, wxe_ref, wye_ref, wzc_ref,
    vxy_ref, vyz_ref, vza_ref, vzb_ref, vxe_ref, vye_ref, vzc_ref, vf_ref,
    s1_ref, t1_ref, s2_ref, t2_ref, const_ref,
    taps, folds,
):
    c = conv1.shape[-1]
    part_z = odd("gz")

    def along_z(i):
        return part_z * i + (1 - part_z) * (2 - i)

    def spread(vector, rows, cols):
        pick = iota((rows, c), 0) % c == iota((rows, c), 1)
        column = jnp.sum(jnp.where(pick, vector, 0.0), axis=1, keepdims=True)
        return jnp.broadcast_to(column, (rows, cols))

    s1_ref[...] = spread(scale1[...], *s1_ref.shape)
    t1_ref[...] = spread(shift1[...], *t1_ref.shape)
    s2_ref[...] = spread(scale2[...], *s2_ref.shape)
    t2_ref[...] = spread(bias1[...] * scale2[...] + shift2[...], *t2_ref.shape)
    const = jnp.sum(flow[...].astype(F32) * bias2[...], axis=1, keepdims=True)
    half = const_ref.shape[0] // 2
    for k in range(2):
        const_ref[k * half : (k + 1) * half] = jnp.broadcast_to(const[k : k + 1], (half, const_ref.shape[1]))

    def tile_of(cols):
        return (iota((c, cols), 0) == iota((c, cols), 1) % c).astype(F32).astype(BF16)

    tile = tile_of(taps.shape[-1])
    short = tile_of(folds.shape[-1])
    for i in range(3):
        for j in range(3):
            taps[i, j] = matmul(conv1[i, j], tile)
            both = matmul(flow[...], conv2[i, j])
            high = both.astype(BF16)
            low = (both - high.astype(F32)).astype(BF16)
            folds[i, j, 0] = matmul(high, short)
            folds[i, j, 1] = matmul(low, short)

    def banded(ref, pick):
        rows, cols = ref.shape
        group = cols // 3
        lane = iota((c, cols), 1)
        slot = lane % group // c
        for a in range(rows // c):
            value = jnp.zeros((c, cols), F32)
            for g in range(3):
                for i in range(3):
                    value = jnp.where((slot == a + i) & (lane // group == g), pick(g, i)[:, :cols], value)
            ref[a * c : (a + 1) * c] = value.astype(BF16)

    banded(wxy_ref, lambda g, i: taps[i, g])
    banded(wyz_ref, lambda g, i: taps[along_z(g), i])
    banded(wza_ref, lambda g, i: taps[along_z(i), g])
    banded(wzb_ref, lambda g, i: taps[along_z(i), g])
    banded(wxe_ref, lambda g, i: taps[i, g])
    banded(wye_ref, lambda g, i: taps[along_z(g), i])
    banded(wzc_ref, lambda g, i: taps[along_z(i), g])

    def banded_flow(ref, pick, place, steps=3):
        cols = ref.shape[1]
        height = ref.shape[0] // 12
        band = place(iota((height, cols), 1) // c) - iota((height, cols), 0)
        for part in range(2):
            for g in range(3):
                for k in range(2):
                    block = jnp.zeros((height, cols), F32)
                    for i in range(steps):
                        row, col = pick(g, i)
                        block = jnp.where(band == i, folds[row, col, part, k : k + 1, :cols], block)
                    at = ((part * 3 + g) * 2 + k) * height
                    ref[at : at + height] = block.astype(BF16)

    middle = vxy_ref.shape[1] // c - 2 * EDGE
    past = vza_ref.shape[1] // c
    banded_flow(vxy_ref, lambda g, i: (i, g), lambda b: b)
    banded_flow(vyz_ref, lambda g, i: (along_z(g), i), lambda b: b)
    banded_flow(vza_ref, lambda g, i: (along_z(i), g), lambda b: b)
    banded_flow(vzb_ref, lambda g, i: (along_z(i), g), lambda b: b + past)
    banded_flow(vxe_ref, lambda g, i: (i, g), lambda b: jnp.where(b < EDGE, b, b + middle))
    banded_flow(vye_ref, lambda g, i: (along_z(g), i), lambda b: jnp.where(b < EDGE, b, b + middle))
    banded_flow(vzc_ref, lambda g, i: (along_z(i), g), lambda b: b, 1)
    cols = vf_ref.shape[1]
    plain = matmul(flow[...], short)
    for k in range(2):
        band = iota((half, cols), 1) // c - iota((half, cols), 0)
        vf_ref[k * half : (k + 1) * half] = jnp.where(band == 0, plain[k : k + 1, :cols], 0.0).astype(BF16)


def shift_right(value):
    return jnp.where(iota(value.shape, 1) == 0, jnp.zeros_like(value), pltpu.roll(value, 1, 1))


def shift_left(value):
    last = value.shape[1] - 1
    return jnp.where(iota(value.shape, 1) == last, jnp.zeros_like(value), pltpu.roll(value, last, 1))


def valid_sides():
    part_z = odd("gz")
    low = (lax.axis_index("gz") > 0).astype(F32)
    high = (lax.axis_index("gz") < lax.axis_size("gz") - 1).astype(F32)
    near = jnp.where(part_z == 1, low, high)
    far = jnp.where(part_z == 1, high, low)
    low_y = (lax.axis_index("gy") > 0).astype(F32)
    high_y = (lax.axis_index("gy") < lax.axis_size("gy") - 1).astype(F32)
    return near, far, low_y, high_y


def y_halos(rows, low_y, high_y):
    part_y = odd("gy")
    valid_even = jnp.where(part_y == 1, low_y, high_y)
    valid_odd = jnp.where(part_y == 1, high_y, low_y)
    return ((1 - part_y) * (rows + HALO), valid_even), (part_y * (rows + HALO), valid_odd)


def normalized(value, s1, t1, valid):
    count, c, cols = value.shape
    size = count * c
    value = jnp.maximum(value.reshape(size, cols).astype(F32) * s1[:size] + t1[:size], 0.0)
    if valid is not None:
        value = value * valid
    value = value.astype(BF16)
    return [v.reshape(count, c, cols) for v in (shift_right(value), value, shift_left(value))]


def set_masks(sm, tm, s2, t2, low_y, high_y):
    size, cols = s2.shape
    c = size // SPAN
    row = iota((size, cols), 0)
    for n, keep in enumerate((row >= 2 * c, row < size - 2 * c)):
        keep = jnp.where(keep, 1.0, high_y if n else low_y)
        sm[n] = s2[...] * keep
        tm[n] = t2[...] * keep


def activate(hidden, scale, shift, c, valid=None):
    value = jnp.maximum(hidden * scale + shift, 0.0)
    if valid is not None:
        value = value * valid
    return value.astype(BF16).reshape(-1, c, value.shape[1])


def stack(pieces):
    return jnp.concatenate([p.reshape(-1, p.shape[-1]) for p in pieces], axis=0)


def two_parts(value):
    half = value.shape[0] // 2
    return value[:half] + value[half:]


def along_x(value):
    value = two_parts(value)
    step = value.shape[0] // 3
    return shift_right(value[:step]) + value[step : 2 * step] + shift_left(value[2 * step :])


def edge_scale(s2, count, first, valid):
    c = s2.shape[0] // SPAN
    row = iota((count * c, s2.shape[1]), 0)
    keep = (row >= first * c) if first > 0 else (row < (count + first) * c)
    return jnp.where(keep, 1.0, valid)


def yz_parts(weights, cells):
    value = two_parts(matmul(weights[...], cells))
    step = value.shape[0] // 3
    return [value[i * step : (i + 1) * step] for i in range(3)]


def layer_parts(layer, flow_xz, flow_xy, flow_yz, base, height):
    parts = [0.5 * flow_xz[0], None, 0.5 * flow_xz[1]]

    def plus(k, value):
        parts[k] = value if parts[k] is None else parts[k] + value

    for i in range(3):
        if layer + i - 1 in flow_yz:
            piece = 0.5 * flow_yz[layer + i - 1][i]
            plus(0, piece[:height])
            plus(1, piece[height:])
    if layer in flow_xy:
        piece = 0.5 * flow_xy[layer]
        plus(1, piece[:height])
        plus(2, piece[height:])
    if base is not None:
        plus(0, base[:height])
        plus(1, 0.5 * (base[:height] + base[height:]))
        plus(2, base[height:])
    return parts


def rim_kernel(
    own, yeven, yodd, wyz, wzc, vyz, vzc, s1, t1, s2, t2, near_ref, corner_ref, unit,
):
    depth, rows, c, cols = own.shape
    for layer in range(HALO):
        near_ref[layer, :rows] = own[layer]
        near_ref[layer, rows : rows + HALO] = yeven[layer]
        near_ref[layer, rows + HALO :] = yodd[layer]
    for layer in range(2):
        for row in range(HALO):
            corner_ref[layer * 2 * HALO + row] = yeven[depth - 1 - layer, row]
            corner_ref[layer * 2 * HALO + HALO + row] = yodd[depth - 1 - layer, row]

    _, _, low_y, high_y = valid_sides()
    (at_even, valid_even), (at_odd, valid_odd) = y_halos(rows, low_y, high_y)

    def place(value, z, y, valid):
        for j, moved in enumerate(normalized(value, s1, t1, valid)):
            unit[j, z, pl.ds(y, value.shape[0])] = moved

    for z in range(3):
        layer = depth - 3 + z
        place(own[layer], z, HALO, None)
        place(yeven[layer], z, at_even, valid_even)
        place(yodd[layer], z, at_odd, valid_odd)
    keeps = (edge_scale(s2, SPAN, 2, low_y), edge_scale(s2, SPAN, -2, high_y))
    act_yz = []
    for w, keep in enumerate(keeps):
        data = stack([unit[1, i, w * SPAN : w * SPAN + WIDE] for i in range(3)])
        act_yz.append(activate(matmul(wyz[...], data), s2[...] * keep, t2[...] * keep, c))
    act_xz = []
    for y in range(rows + 2):
        data = stack([unit[j, z, y + 2] for j in range(3) for z in range(3)])
        act_xz.append(activate(matmul(wzc[...], data), s2[:c], t2[:c], c))
    flow_yz = 0.5 * yz_parts(vyz, stack(act_yz))[0]
    flow_xz = 0.5 * along_x(matmul(vzc[...], stack(act_xz)))
    height = flow_xz.shape[0] // 2
    corner_ref[4 * HALO, :height] = (flow_yz[:height] + flow_xz[:height]).astype(BF16)
    corner_ref[4 * HALO, height:] = flow_yz[height:].astype(BF16)
    corner_ref[4 * HALO + 1, :height] = flow_xz[height:].astype(BF16)
    corner_ref[4 * HALO + 1, height:] = jnp.zeros((height, cols), BF16)


def near_kernel(
    own, near, yeven, yodd, wxy, wyz, wza, vxy, vyz, vza, vf, s1, t1, s2, t2, const,
    mean, tail, unit, feat, act_xy, act_yz, act_xz, sm, tm, fxz,
):
    depth, rows, c, cols = own.shape
    valid_near, _, low_y, high_y = valid_sides()
    (at_even, valid_even), (at_odd, valid_odd) = y_halos(rows, low_y, high_y)
    start = HALO + depth
    first = start - 2

    def place(value, z, y, valid):
        count = value.shape[0]
        if z >= HALO - 1:
            feat[z - HALO + 1, pl.ds(y, count)] = value
        for j, moved in enumerate(normalized(value, s1, t1, valid)):
            if z < first:
                unit[j, z, pl.ds(y, count)] = moved
            else:
                tail[j, z - first, pl.ds(y, count)] = moved

    for z in range(depth):
        place(own[z], HALO + z, HALO, None)
        place(yeven[z], HALO + z, at_even, valid_even)
        place(yodd[z], HALO + z, at_odd, valid_odd)
    for z in range(HALO):
        place(near[z, :rows], HALO - 1 - z, HALO, valid_near)
        place(near[z, rows : rows + HALO], HALO - 1 - z, at_even, valid_near * valid_even)
        place(near[z, rows + HALO :], HALO - 1 - z, at_odd, valid_near * valid_odd)
    set_masks(sm, tm, s2, t2, low_y, high_y)

    def read(j, z, y):
        return unit[j, z, y] if z < first else tail[j, z - first, y]

    wide = rows + 4
    for n, z in enumerate(range(2, start)):
        for w in range(wide // SPAN):
            data = stack([read(j, z, slice(w * SPAN, w * SPAN + WIDE)) for j in range(3)])
            act_xy[n, w * SPAN : (w + 1) * SPAN] = activate(matmul(wxy[...], data), sm[w], tm[w], c)
    for n, z in enumerate(range(1, first + 1)):
        valid = valid_near if z < HALO else None
        for w in range(wide // SPAN):
            data = stack([read(1, z + i - 1, slice(w * SPAN, w * SPAN + WIDE)) for i in range(3)])
            act_yz[n, w * SPAN : (w + 1) * SPAN] = activate(matmul(wyz[...], data), sm[w], tm[w], c, valid)
    count = depth + 1
    keep = edge_scale(s2, count, 2, valid_near)
    scale, shift = s2[: count * c] * keep, t2[: count * c] * keep
    for y in range(rows + 2):
        data = stack([read(j, z, y + 2) for j in range(3) for z in range(depth + 3)])
        act_xz[y] = activate(matmul(wza[...], data), scale, shift, c)
    for y in range(rows + 2):
        flow = along_x(matmul(vza[...], act_xz[y].reshape(-1, cols)))
        half = flow.shape[0] // 2
        for k in range(2):
            fxz[k, :, y, :] = flow[k * half : (k + 1) * half]
    height = mean.shape[2]
    flow_xy = {z: along_x(matmul(vxy[...], act_xy[n].reshape(-1, cols))) for n, z in enumerate(range(2, start))}
    flow_yz = {z: yz_parts(vyz, act_yz[n].reshape(-1, cols)) for n, z in enumerate(range(1, first + 1))}
    for layer in range(2, start):
        at = layer - 2
        base = matmul(vf[...], feat[at, 2 : rows + 4].reshape(-1, cols)) + const[...]
        for k, value in enumerate(layer_parts(layer, (fxz[0, at], fxz[1, at]), flow_xy, flow_yz, base, height)):
            mean[k, at] = value


def mid_kernel(
    last, far, tail, wxy, wyz, wzb, vxy, vyz, vzb, vf, s1, t1, s2, t2, const,
    more, face, fxz,
):
    _, rows, c, cols = far.shape
    _, valid_far, _, _ = valid_sides()
    for z in range(2):
        for j, moved in enumerate(normalized(far[z], s1, t1, valid_far)):
            face[j, z] = moved

    def read(j, z, y):
        return tail[j, z, y + HALO] if z < 2 else face[j, z - 2, y]

    keep = edge_scale(s2, 2, -1, valid_far)
    scale, shift = s2[: 2 * c] * keep, t2[: 2 * c] * keep
    none = jnp.zeros((c, cols), BF16)
    gap = jnp.zeros((EDGE * c, cols), BF16)

    def middle(cells):
        return jnp.concatenate([gap, cells.reshape(-1, cols), gap], axis=0)

    inner = slice(HALO, HALO + rows)
    data = stack([face[j, 0] for j in range(3)])
    act_xy = activate(matmul(wxy[...], data), s2[...], t2[...], c)
    act_yz = []
    for z in range(1, 3):
        data = stack([tail[1, i, inner] if i < 2 else face[1, i - 2] for i in range(z - 1, z + 2)])
        act_yz.append(activate(matmul(wyz[...], data), s2[...], t2[...], c, valid_far if z > 1 else None))
    act_xz = []
    for y in range(rows):
        data = stack([p for j in range(3) for p in (*(read(j, z, y) for z in range(4)), none)])
        act_xz.append(activate(matmul(wzb[...], data)[: 2 * c], scale, shift, c))
    flow_xy = {2: along_x(matmul(vxy[...], middle(act_xy)))}
    flow_yz = {z: yz_parts(vyz, middle(act_yz[z - 1])) for z in range(1, 3)}
    flow_xz = [along_x(matmul(vzb[...], stack([cells, none]))) for cells in act_xz]
    fxz[...] = jnp.zeros_like(fxz)
    for y, flow in enumerate(flow_xz):
        half = flow.shape[0] // 2
        for k in range(2):
            fxz[k, :, y + 1, :] = flow[k * half : (k + 1) * half]
    height = more.shape[2]
    for layer in range(3):
        base = None
        if layer == 2:
            cells = jnp.concatenate([gap[:c], far[0].reshape(-1, cols), gap[:c]], axis=0)
            base = matmul(vf[...], cells) + const[...]
        at = last + layer - 2
        for k, value in enumerate(layer_parts(layer, (fxz[0, at], fxz[1, at]), flow_xy, flow_yz, base, height)):
            more[k, layer] = value


def far_kernel(
    corner, tail, face, mean, more, wzb, wxe, wye, vzb, vxe, vye, vf, s1, t1, s2, t2,
    out, unit, fxz, feat, total,
):
    _, depth, rows, cols = out.shape
    c = corner.shape[1]
    valid_near, valid_far, low_y, high_y = valid_sides()
    (at_even, valid_even), (at_odd, valid_odd) = y_halos(rows, low_y, high_y)
    start = HALO + depth
    first = start - 2

    def place(value, z, y, valid):
        count = value.shape[0]
        if z == 0:
            feat[pl.ds(y, count)] = value
        for j, moved in enumerate(normalized(value, s1, t1, valid)):
            unit[j, z, pl.ds(y, count)] = moved

    for z in range(2):
        at = z * 2 * HALO
        place(corner[at : at + HALO], z, at_even, valid_far * valid_even)
        place(corner[at + HALO : at + 2 * HALO], z, at_odd, valid_far * valid_odd)

    def read(j, z, y):
        if z < start:
            return tail[j, z - first, y]
        return face[j, z - start, y - HALO] if HALO <= y < HALO + rows else unit[j, z - start, y]

    low, high = range(EDGE + 2), range(rows + 1, rows + 6)
    keeps = (edge_scale(s2, EDGE, 2, low_y), edge_scale(s2, EDGE, -2, high_y))
    scales = [s2[: EDGE * c] * keep for keep in keeps]
    shifts = [t2[: EDGE * c] * keep for keep in keeps]
    keep = edge_scale(s2, 2, -1, valid_far)
    scale, shift = s2[: 2 * c] * keep, t2[: 2 * c] * keep
    none = jnp.zeros((c, cols), BF16)
    act_xy = []
    for side, window in enumerate((low, high)):
        data = stack([read(j, start, y) for j in range(3) for y in window])
        act_xy.append(activate(matmul(wxe[...], data), scales[side], shifts[side], c))
    act_yz = {}
    for z in range(first + 1, start + 1):
        for side, window in enumerate((low, high)):
            data = stack([read(1, z + i - 1, y) for i in range(3) for y in window])
            valid = valid_far if z >= start else None
            act_yz[z, side] = activate(matmul(wye[...], data), scales[side], shifts[side], c, valid)
    act_xz = []
    for y in (0, rows + 1):
        data = stack([p for j in range(3) for p in (*(read(j, first + z, y + 2) for z in range(4)), none)])
        act_xz.append(activate(matmul(wzb[...], data)[: 2 * c], scale, shift, c))
    flow_xy = {start: along_x(matmul(vxe[...], stack(act_xy)))}
    flow_yz = {z: yz_parts(vye, stack([act_yz[z, 0], act_yz[z, 1]])) for z in range(first + 1, start + 1)}
    flow_xz = [along_x(matmul(vzb[...], stack([cells, none]))) for cells in act_xz]
    fxz[...] = jnp.zeros_like(fxz)
    for y, flow in zip((0, rows + 1), flow_xz):
        half = flow.shape[0] // 2
        for k in range(2):
            fxz[k, :, y, :] = flow[k * half : (k + 1) * half]
    gap = jnp.zeros((rows * c, cols), BF16)
    base = matmul(vf[...], jnp.concatenate([feat[2], gap, feat[rows + 3]], axis=0))

    height = mean.shape[2]
    spot = iota((height, cols), 0)
    inside_y = jnp.where(spot == 0, low_y, jnp.where(spot == rows + 1, high_y, jnp.where(spot < rows + 1, 1.0, 0.0)))
    for layer in range(2, start + 1):
        at = layer - 2
        keep = inside_y * valid_near if at == 0 else inside_y * valid_far if layer == start else inside_y
        if layer < first:
            for k in range(3):
                total[k, at] = mean[k, at] * keep
        else:
            added = layer_parts(
                layer, (fxz[0, at], fxz[1, at]), flow_xy, flow_yz, base if layer == start else None, height
            )
            for k in range(3):
                value = more[k, layer - first] + added[k]
                if layer < start:
                    value = value + mean[k, at]
                else:
                    half = slice(k % 2 * height, (k % 2 + 1) * height)
                    value = value + corner[4 * HALO + k // 2, half].astype(F32)
                total[k, at] = value * keep
    part_z = odd("gz")
    for k in range(3):
        for z in range(depth):
            value = 0.25 * (total[k, z] + total[k, z + 2]) + 0.5 * total[k, z + 1]
            value = 0.25 * (value[:rows] + value[2 : rows + 2]) + 0.5 * value[1 : rows + 1]
            value = 0.25 * (shift_right(value) + shift_left(value)) + 0.5 * value
            out[k, part_z * z + (1 - part_z) * (depth - 1 - z)] = value


def shards(
    features, scale_first, shift_first, conv_first, bias_first,
    scale_second, shift_second, conv_second, bias_second, flow_weight,
):
    c, depth, rows, cols = features.shape
    shape = jax.ShapeDtypeStruct
    cells = functools.partial(shape, dtype=BF16)
    side = cells((depth, HALO, c, cols))
    params = [
        scale_first[None], shift_first[None], conv_first, bias_first[None],
        scale_second[None], shift_second[None], conv_second, bias_second[None], flow_weight,
    ]
    params = [pltpu.with_memory_space_constraint(p, pltpu.HBM) for p in params]
    own, send_even, send_odd, send_far, *params = call(
        pack_kernel,
        [cells((depth, rows, c, cols)), side, side, cells((2, rows, c, cols))]
        + [shape(p.shape, p.dtype) for p in params],
        [pltpu.with_memory_space_constraint(features, pltpu.HBM), *params],
        2 * features.size * c * rows, 6,
        [pltpu.VMEM(features.shape, BF16), pltpu.SemaphoreType.DMA((len(params) + 1,))],
        HBM,
    )
    yeven = swap(send_even, "gy", 0)
    yodd = swap(send_odd, "gy", 1)
    far = swap(send_far, "gz", 1)

    broad = rows + 2 * HALO
    high = -(-(rows + 2) // 8) * 8
    deep = -(-(depth + 2) // 8) * 8
    wxy, wyz, wza, wzb, wxe, wye, wzc, vxy, vyz, vza, vzb, vxe, vye, vzc, vf, *rest = call(
        weights_kernel,
        [
            cells((SPAN * c, 3 * WIDE * c)),
            cells((SPAN * c, 3 * WIDE * c)),
            cells(((depth + 1) * c, 3 * (depth + 3) * c)),
            *[cells((EDGE * c, 3 * (EDGE + 2) * c))] * 3,
            cells((c, 9 * c)),
            cells((12 * high, (rows + 4) * c)),
            cells((12 * high, (rows + 4) * c)),
            cells((12 * deep, (depth + 1) * c)),
            cells((12 * deep, EDGE * c)),
            *[cells((12 * high, 2 * EDGE * c))] * 2,
            cells((12 * high, (rows + 2) * c)),
            cells((2 * high, (rows + 2) * c)),
            shape((rows * c, cols), F32),
            shape((rows * c, cols), F32),
            shape((SPAN * c, cols), F32),
            shape((SPAN * c, cols), F32),
            shape((2 * high, cols), F32),
        ],
        params,
        2 * 10**9, 10,
        [
            pltpu.VMEM((3, 3, c, 3 * WIDE * c), F32),
            pltpu.VMEM((3, 3, 2, 2, (rows + 4) * c), F32),
        ],
    )
    assert c == 2 * high
    send_near, send_corner = call(
        rim_kernel,
        [cells((HALO, broad, c, cols)), cells((4 * HALO + 2, c, cols))],
        [own, yeven, yodd, wyz, wzc, vyz, vzc, *rest[:4]],
        10**8, 10,
        [pltpu.VMEM((3, 3, broad, c, cols), BF16)],
    )
    corner = swap(send_corner, "gz", 1)
    near = swap(send_near, "gz", 0)

    mean, tail = call(
        near_kernel,
        [shape((3, depth + 1, high, cols), F32), cells((3, 2, broad, c, cols))],
        [own, near, yeven, yodd, wxy, wyz, wza, vxy, vyz, vza, vf, *rest],
        6 * 10**9, 24,
        [
            pltpu.VMEM((3, depth + 1, broad, c, cols), BF16),
            pltpu.VMEM((depth + 1, broad, c, cols), BF16),
            pltpu.VMEM((depth + 1, rows + 4, c, cols), BF16),
            pltpu.VMEM((depth + 1, rows + 4, c, cols), BF16),
            pltpu.VMEM((rows + 2, depth + 1, c, cols), BF16),
            pltpu.VMEM((2, SPAN * c, cols), F32),
            pltpu.VMEM((2, SPAN * c, cols), F32),
            pltpu.VMEM((2, deep, high, cols), F32),
        ],
    )
    more, face = call(
        functools.partial(mid_kernel, depth + 1),
        [shape((3, 3, high, cols), F32), cells((3, 2, rows, c, cols))],
        [far, tail, wxy, wyz, wzb, vxy, vyz, vzb, vf, *rest],
        3 * 10**9, 12,
        [pltpu.VMEM((2, deep, high, cols), F32)],
    )
    (out,) = call(
        far_kernel,
        [shape((3, depth, rows, cols), F32)],
        [corner, tail, face, mean, more, wzb, wxe, wye, vzb, vxe, vye, vf, *rest[:4]],
        2 * 10**9, 16,
        [
            pltpu.VMEM((3, HALO, broad, c, cols), BF16),
            pltpu.VMEM((2, deep, high, cols), F32),
            pltpu.VMEM((broad, c, cols), BF16),
            pltpu.VMEM((3, depth + 2, high, cols), F32),
        ],
    )
    return out


def solution(mesh):
    return jax.shard_map(
        shards,
        mesh=mesh,
        in_specs=(P(None, "gz", "gy", None), P(), P(), P(), P(), P(), P(), P(), P(), P()),
        out_specs=P(None, "gz", "gy", None),
        check_vma=False,
    )
```
